32 devices in a mesh: row: 4 (over y, core), col: 8 (over z, x).
Axes of the slice: x: 2, y: 2, z: 4, core: 2. Of those that a mesh axis runs over, the one named last changes fastest.
Arguments:
- sources: bfloat16 [4, 8, 4, 256, 256], P('row', 'col'), may hold values from -6 to 6
- history: bfloat16 [4, 8, 8, 256, 256], P(None, 'col'), may hold values from -4 to 4
- inverse_diagonal: float32 [4, 8, 256], P('row', 'col'), may hold values from 0.3 to 0.6
- far_cores: bfloat16 [4, 8, 32, 4, 8, 8, 32], P('row', None, None, None, 'col'), may hold values from -0.09375 to 0.09375
- target_basis: bfloat16 [4, 8, 256, 32], P('row', 'col'), may hold values from -1 to 1
- source_basis: bfloat16 [4, 8, 256, 32], P(None, 'col'), may hold values from -0.375 to 0.375
- near_blocks: bfloat16 [4, 8, 3, 256, 8, 256], P('row', 'col'), may hold values from -0.078125 to 0.078125
- near_tile: int32 [4, 8, 3], P('row', 'col'), may hold values from 0 to 3
- near_count: int32 [4, 8], P('row', 'col'), may hold values from 1 to 3, as said below
Outputs:
- new_steps: bfloat16 [4, 8, 4, 256, 256], P('row', 'col')
- energies: float32 [4, 256], replicated
The draws below stay inside these ranges and needn't reach their ends.
Inputs may be any that keep to these rules, and one draw needn't show every extreme that they name: Only slots below near_count are used; in every draw some tile has all 3 slots live.
All inputs are finite; a program needn't handle non-finite values.
Results may differ from the reference program's by a relative error of at most 0.011.
Values may be sent and summed in bfloat16 or wider, within the bound.
A program may use at most 192 MiB of HBM per device.

```python
import math
import jax
import jax.numpy as jnp
from jax import lax

TILE = 256
RANK = 32
LAGS = 8
STEPS = 4
SLOTS = 3
FIELDS = 256
PANELS = 8192
N_ROW = 4
N_COL = 8


def draw_near_count(key, part):
    first_key, other_key = jax.random.split(jax.random.fold_in(key, 7))
    counts = jax.random.randint(first_key, (N_ROW * N_COL,), 1, SLOTS + 1)
    chosen = jax.random.randint(other_key, (), 0, N_ROW * N_COL)
    counts = counts.at[chosen].set(SLOTS)
    return counts.reshape(N_ROW, N_COL).astype(jnp.int32)


def with_ends(values, own_key, smallest, largest):
    longest = values.shape.index(max(values.shape))
    spots = []
    for shift in (0, 1):
        where = [jax.random.randint(jax.random.fold_in(own_key, axis), (), 0, length) for axis, length in enumerate(values.shape)]
        where[longest] = (where[longest] + shift) % values.shape[longest]
        spots.append(tuple(where))
    return values.at[spots[0]].set(smallest).at[spots[1]].set(largest)


def strengthened(array, key, source, target, parts, factor):
    def block_of(position):
        return (jnp.arange(array.shape[position]) // (array.shape[position] // parts)).reshape((-1,) + (1,) * (array.ndim - 1 - position))

    first = jax.random.permutation(key, parts)[block_of(target)]
    second = (block_of(target) + parts // 2) % parts
    return jnp.where((block_of(source) == first) | (block_of(source) == second), factor * array, array)


def level_of(rng, shape, shards, smallest, top_value):
    def one(dim, blocks):
        draws = jax.random.uniform(jax.random.fold_in(jax.random.fold_in(rng, 6), dim), (blocks,), jnp.float32, smallest / len(shards), top_value / len(shards))
        return jnp.repeat(jnp.exp(draws), shape[dim] // blocks).reshape((-1,) + (1,) * (len(shape) - dim - 1))

    loudness = one(*shards[0])
    for cut in shards[1:]:
        loudness = loudness * one(*cut)
    return loudness


def noise(key, shape, spread, reach, cuts=(), held_as=jnp.bfloat16):
    factor_of = level_of(key, shape, cuts, -0.22, 0.18) if cuts else 1.0
    drawn = jax.random.normal(key, shape, jnp.float32) * spread * factor_of
    return jnp.minimum(jnp.maximum(drawn, -reach), reach).astype(held_as)


def noise_with(stream_key, shape, scale, limit, pieces, heavy, kind=jnp.bfloat16):
    result = scale * jax.random.normal(stream_key, shape, jnp.float32)
    if pieces:
        result = result * level_of(stream_key, shape, pieces, -0.22, 0.18)
    return jnp.clip(strengthened(result, jax.random.fold_in(stream_key, 3), *heavy), -limit, limit).astype(kind)


def setup_inputs(seed: int = 0) -> dict:
    seeds = jax.random.split(jax.random.key(seed), 10)
    return {
        "sources": noise(seeds[0], (N_ROW, N_COL, STEPS, TILE, FIELDS), 1.0, 6.0, ((0, 4), (1, 8))),
        "history": noise(seeds[1], (N_ROW, N_COL, LAGS, TILE, FIELDS), 0.5, 4.0, ((1, 8),)),
        "inverse_diagonal": jnp.clip(jnp.exp(math.log(0.6) - 0.6931472 * jax.random.uniform(seeds[2], (N_ROW, N_COL, TILE), jnp.float32) ** level_of(seeds[2], (N_ROW, N_COL, TILE), ((0, 4), (1, 8)), -0.2, 0.2)), 0.3, 0.6),
        "far_cores": noise_with(seeds[3], (N_ROW, N_COL, RANK, N_ROW, N_COL, LAGS, RANK), (N_ROW * N_COL * LAGS * RANK) ** -0.5, 0.09375, ((0, 4), (4, 8)), (4, 1, 8, 2.0)),
        "target_basis": noise(seeds[4], (N_ROW, N_COL, TILE, RANK), RANK ** -0.5, 1.0, ((0, 4), (1, 8))),
        "source_basis": noise(seeds[5], (N_ROW, N_COL, TILE, RANK), TILE ** -0.5, 0.375, ((1, 8),)),
        "near_blocks": noise(seeds[6], (N_ROW, N_COL, SLOTS, TILE, LAGS, TILE), (SLOTS * LAGS * TILE) ** -0.5, 0.078125, ((0, 4), (1, 8))),
        "near_tile": with_ends(jax.random.randint(seeds[7], (N_ROW, N_COL, SLOTS), 0, N_ROW), jax.random.fold_in(seeds[7], 1), 0, N_ROW - 1).astype(jnp.int32),
        "near_count": draw_near_count(jax.random.fold_in(seeds[9], 71), 0),
    }


def project(source_basis, blocks):
    return jnp.einsum("ijta,ijktx->ijkax", source_basis.astype(jnp.float32), blocks.astype(jnp.float32)).astype(jnp.bfloat16)


def reference(sources, history, inverse_diagonal, far_cores, target_basis, source_basis, near_blocks, near_tile, near_count):
    row_count = history.shape[0]
    col_count = history.shape[1]
    past = history
    projected = project(source_basis, past)
    flat_blocks = near_blocks.reshape(row_count * col_count, SLOTS, TILE, LAGS * TILE)
    flat_tiles = near_tile.reshape(row_count * col_count, SLOTS)
    flat_counts = near_count.reshape(row_count * col_count)
    col_ids = (jnp.arange(row_count * col_count, dtype=jnp.int32) % col_count).astype(jnp.int32)
    outputs = []
    energy_rows = []
    for moment in range(STEPS):
        stacked = projected.reshape(row_count * col_count * LAGS * RANK, FIELDS)

        def row_cores(cores_row):
            matrix = cores_row.reshape(col_count * RANK, row_count * col_count * LAGS * RANK)
            summed = jnp.dot(matrix, stacked, preferred_element_type=jnp.float32)
            return summed.astype(jnp.bfloat16).reshape(col_count, RANK, FIELDS)

        core_now = lax.map(row_cores, far_cores)
        far = jnp.einsum("ijta,ijax->ijtx", target_basis.astype(jnp.float32), core_now.astype(jnp.float32))

        def near_tile_sum(inputs):
            blocks, tiles, count, col_id = inputs
            column = lax.dynamic_index_in_dim(past, col_id, 1, keepdims=False)
            total = jnp.zeros((TILE, FIELDS), jnp.float32)
            for slot in range(SLOTS):
                source = lax.dynamic_index_in_dim(column, tiles[slot], 0, keepdims=False).reshape(LAGS * TILE, FIELDS)
                term = jnp.dot(blocks[slot], source, preferred_element_type=jnp.float32)
                total = total + jnp.where(slot < count, term, jnp.zeros_like(term))
            return total

        near = lax.map(near_tile_sum, (flat_blocks, flat_tiles, flat_counts, col_ids)).reshape(row_count, col_count, TILE, FIELDS)
        fresh = (inverse_diagonal[:, :, :, None] * (sources[:, :, moment].astype(jnp.float32) - far - near)).astype(jnp.bfloat16)
        outputs.append(fresh)
        energy_rows.append(jnp.sum(jnp.square(fresh.astype(jnp.float32)), axis=(0, 1, 2)) / PANELS)
        past = jnp.concatenate([fresh[:, :, None], past[:, :, :-1]], axis=2)
        projected = jnp.concatenate([project(source_basis, fresh[:, :, None]), projected[:, :, :-1]], axis=2)
    return jnp.stack(outputs, axis=2), jnp.stack(energy_rows, axis=0)
```

```python
import functools

import jax
import jax.numpy as jnp
from jax import lax
from jax.experimental import pallas as pl
from jax.experimental.pallas import tpu as pltpu
from jax.sharding import PartitionSpec as P

MESH = pl.DeviceIdType.MESH
F32 = jnp.float32
BF16 = jnp.bfloat16


def march(
    rows,
    cols,
    panel_total,
    tiles_hbm,
    count_hbm,
    basis_hbm,
    history_hbm,
    cores_hbm,
    near_hbm,
    target_hbm,
    scaling_hbm,
    sources_hbm,
    steps_ref,
    energy_ref,
    tiles_ref,
    count_ref,
    basis,
    history,
    cores,
    near_blocks,
    target,
    scaling_row,
    sources,
    scaling,
    cores_raw,
    near_raw,
    stage,
    past_proj,
    fresh_tiles,
    fresh_proj,
    core_out,
    core_in,
    near_sum,
    partial_sum,
    energy_own,
    energy_early,
    energy_last,
    load_sems,
    history_sems,
    tile_send,
    tile_recv,
    pass_send,
    pass_recv,
    proj_send,
    proj_recv,
    core_send,
    core_recv,
    energy_send,
    energy_recv,
):
    step_count = sources.shape[0]
    lag_count, _, rank, fields = past_proj.shape
    tile = history.shape[2]
    slot_count = near_blocks.shape[0]
    width = rows * rank
    my_row = lax.axis_index("row")
    my_col = lax.axis_index("col")
    partner = my_row + 1 - 2 * lax.rem(my_row, 2)

    def row_peer(d):
        return lax.rem(my_row + d, rows)

    def col_peer(d):
        return lax.rem(my_col + d, cols)

    loads = [
        pltpu.make_async_copy(src, dst, load_sems.at[n])
        for n, (src, dst) in enumerate(
            (
                (basis_hbm, basis),
                (cores_hbm, cores_raw),
                (near_hbm, near_raw),
                (target_hbm, target),
                (scaling_hbm, scaling_row),
                (sources_hbm, sources),
                (tiles_hbm, tiles_ref),
                (count_hbm, count_ref),
            )
        )
    ]

    pairs = [(lag, min(2, lag_count - lag)) for lag in range(0, lag_count, 2)]

    def history_load(index):
        first, length = pairs[index]
        return pltpu.make_async_copy(
            history_hbm.at[:, first:first + length],
            history.at[:, first:first + length],
            history_sems.at[index],
        )

    def wait_bytes(ref, sem):
        pltpu.make_async_copy(ref, ref, sem).wait()

    loads[1].start()
    loads[0].start()
    for index in range(len(pairs)):
        history_load(index).start()

    barrier = pltpu.get_barrier_semaphore()
    peers = [(a, b) for a in range(rows) for b in range(cols) if a or b]

    def greet(index, carry):
        pl.semaphore_signal(
            barrier, inc=1, device_id=(row_peer(index // cols), col_peer(lax.rem(index, cols))),
            device_id_type=MESH,
        )
        return carry

    lax.fori_loop(1, rows * cols, greet, 0)

    def row_copy(src, dst, send, recv, to):
        return pltpu.make_async_remote_copy(
            src_ref=src, dst_ref=dst, send_sem=send, recv_sem=recv,
            device_id={"row": to}, device_id_type=MESH,
        )

    def col_copy(src, dst, send, recv, to):
        return pltpu.make_async_remote_copy(
            src_ref=src, dst_ref=dst, send_sem=send, recv_sem=recv,
            device_id={"col": to}, device_id_type=MESH,
        )

    def proj_copy(n, owner, d):
        return row_copy(
            fresh_proj.at[n, owner], fresh_proj.at[n, owner],
            proj_send.at[n], proj_recv.at[n], row_peer(d),
        )

    def tile_copy(n, owner, d):
        return row_copy(
            fresh_tiles[n].at[owner], fresh_tiles[n].at[owner],
            tile_send.at[n], tile_recv.at[n, owner // 2], row_peer(d),
        )

    def pass_copy(n, owner):
        return row_copy(
            fresh_tiles[n].at[owner], fresh_tiles[n].at[owner],
            pass_send.at[n], pass_recv.at[n], partner,
        )

    def core_copy(n, d):
        to = col_peer(d)
        return col_copy(
            core_out.at[n, to], core_in.at[n, my_col],
            core_send.at[n], core_recv.at[n], to,
        )

    me = my_row * cols + my_col

    def energy_copy(last, owner, d):
        return pltpu.make_async_remote_copy(
            src_ref=energy_own.at[step_count - 1] if last else energy_own.at[0:step_count - 1],
            dst_ref=energy_last.at[owner] if last else energy_early.at[owner],
            send_sem=energy_send.at[last],
            recv_sem=energy_recv.at[last],
            device_id=(row_peer(peers[d][0]), col_peer(peers[d][1])),
            device_id_type=MESH,
        )

    def far_base(n):
        depth = lag_count - n
        total = jnp.dot(
            cores[:, n * width:],
            past_proj[0:depth].reshape(depth * width, fields),
            preferred_element_type=F32,
        )
        for lag in range(1, n):
            total += jnp.dot(
                cores[:, lag * width:(lag + 1) * width],
                fresh_proj[n - 1 - lag].reshape(width, fields),
                preferred_element_type=F32,
            )
        return total

    def near_base(n):
        depth = lag_count - n

        def add_slot(slot, carry):
            where = tiles_ref[0, 0, slot]
            value = jnp.dot(
                near_blocks[slot, :, n * tile:],
                history[where, 0:depth].reshape(depth * tile, fields),
                preferred_element_type=F32,
            )
            for lag in range(1, n):
                value += jnp.dot(
                    near_blocks[slot, :, lag * tile:(lag + 1) * tile],
                    fresh_tiles[n - 1 - lag][where],
                    preferred_element_type=F32,
                )
            near_sum[n] += value
            return carry

        near_sum[n] = jnp.zeros((tile, fields), F32)
        lax.fori_loop(0, slot_count, add_slot, 0)

    def near_fresh(n):
        total = near_sum[n]
        for slot in range(slot_count):
            total += jnp.dot(
                near_blocks[slot, :, 0:tile],
                fresh_tiles[n - 1][tiles_ref[0, 0, slot]],
                preferred_element_type=F32,
            )
        near_sum[n] = sources[n].astype(F32) - total

    lanes = stage.shape[2]
    block = stage.shape[1] // lag_count

    def spread(value, base=0):
        for c in range(value.shape[1] // lanes):
            stage[base + c] = value[:, c * lanes:(c + 1) * lanes]

    def pick(lag, c):
        return stage[c, pl.ds(lag, block, stride=lag_count), :].astype(BF16)

    def pack_cores(g):
        here = pl.ds(g * block, block)
        base = g % 2 * (width // lanes)
        total = None
        for p in range(rows):
            value = cores_raw[here, p].astype(F32).reshape(block * lag_count, rank).astype(BF16)
            place = (
                lax.broadcasted_iota(jnp.int32, (rank, width), 1)
                == lax.broadcasted_iota(jnp.int32, (rank, width), 0) + p * rank
            )
            term = jnp.dot(
                value, place.astype(F32).astype(BF16), preferred_element_type=F32
            )
            total = term if total is None else total + term
        spread(total, base)
        for lag in range(lag_count):
            for c in range(width // lanes):
                first = lag * width + c * lanes
                cores[here, first:first + lanes] = pick(lag, base + c)

    def pack_near(index, carry):
        slot = index // (tile // block)
        here = pl.ds(pl.multiple_of(lax.rem(index, tile // block) * block, block), block)
        spread(near_raw[slot, here].astype(F32).reshape(block * lag_count, tile))
        for lag in range(lag_count):
            for c in range(tile // lanes):
                first = lag * tile + c * lanes
                near_blocks[slot, here, first:first + lanes] = jnp.where(
                    slot < count_ref[0, 0], pick(lag, c), jnp.zeros((block, lanes), BF16)
                )
        return carry

    loads[1].wait()
    for load in loads[2:]:
        load.start()
    for g in range(cores.shape[0] // block):
        pack_cores(g)
    loads[0].wait()
    for index, (first, length) in enumerate(pairs):
        history_load(index).wait()
        for lag in range(first, first + length):
            for p in range(rows):
                past_proj[lag, p] = jnp.dot(
                    basis[p], history[p, lag], preferred_element_type=F32
                ).astype(BF16)

    far_first = sorted(range(1, cols), key=lambda d: -min(d, cols - d))
    for n in range(step_count):
        if n == 0:
            partial = far_base(0)
        else:
            wait_bytes(fresh_proj.at[n - 1, 0:rows - 1], proj_recv.at[n - 1])
            partial = partial_sum[...] + jnp.dot(
                cores[:, 0:width],
                fresh_proj[n - 1].reshape(width, fields),
                preferred_element_type=F32,
            )
        core_out[n] = partial.astype(BF16).reshape(cols, rank, fields)
        if n == 0:
            pl.semaphore_wait(barrier, rows * cols - 1)
        for d in far_first:
            core_copy(n, d).start()
        if n + 1 == step_count:
            for d in range(len(peers)):
                energy_copy(0, me, d).start()
        if n == 0:
            for load in (loads[2], *loads[6:]):
                load.wait()
            lax.fori_loop(0, slot_count * (tile // block), pack_near, 0)
            near_base(0)
            for load in loads[3:6]:
                load.wait()
            scaling[...] = jnp.transpose(jnp.broadcast_to(scaling_row[...], (fields, tile)))
            near_sum[0] = sources[0].astype(F32) - near_sum[0]
        else:
            near_base(n)
            for d in range(2, rows, 2):
                tile_copy(n - 1, row_peer(d), d).wait_recv()
                pass_copy(n - 1, row_peer(d)).start()
            tile_copy(n - 1, partner, 1).wait_recv()
            wait_bytes(fresh_tiles[n - 1].at[0:rows // 2 - 1], pass_recv.at[n - 1])
            near_fresh(n)
        core = core_out[n, my_col].astype(F32)
        wait_bytes(core_in.at[n, 0:cols - 1], core_recv.at[n])
        for d in range(1, cols):
            core += core_in[n, col_peer(d)].astype(F32)
        far = lax.dot_general(
            target[...], core.astype(BF16), (((0,), (0,)), ((), ())),
            preferred_element_type=F32,
        )
        fresh = (scaling[...] * (near_sum[n] - far)).astype(BF16)
        if n + 1 < step_count:
            fresh_tiles[n][my_row] = fresh
            row_copy(
                fresh_tiles[n].at[my_row], fresh_tiles[n].at[my_row],
                tile_send.at[n], tile_recv.at[n, my_row // 2], partner,
            ).start()
            fresh_proj[n, my_row] = jnp.dot(
                basis[my_row], fresh, preferred_element_type=F32
            ).astype(BF16)
            for d in range(1, rows):
                proj_copy(n, my_row, d).start()
            for d in range(2, rows, 2):
                tile_copy(n, my_row, d).start()
            steps_ref[n] = fresh
        else:
            steps_ref[n] = fresh
        energy_own[n] = (
            jnp.sum(jnp.square(fresh.astype(F32)), axis=0, keepdims=True) / panel_total
        )
        if n + 1 < step_count:
            partial_sum[...] = far_base(n + 1)

    for d in range(len(peers)):
        energy_copy(1, me, d).start()
    energy_early[me] = energy_own[0:step_count - 1]
    energy_last[me] = energy_own[step_count - 1]
    for last, where in ((0, energy_early), (1, energy_last)):
        wait_bytes(where.at[0:len(peers)], energy_recv.at[last])
        total = where[0]
        for origin in range(1, rows * cols):
            total += where[origin]
        if last:
            energy_ref[step_count - 1:step_count, :] = total
        else:
            for n in range(step_count - 1):
                energy_ref[n:n + 1, :] = total[n]

    for n in range(step_count):
        wait_bytes(core_in.at[n, 0:cols - 1], core_send.at[n])
        if n + 1 < step_count:
            wait_bytes(fresh_proj.at[n, 0:rows - 1], proj_send.at[n])
            wait_bytes(fresh_tiles[n].at[0:rows // 2], tile_send.at[n])
            wait_bytes(fresh_tiles[n].at[0:rows // 2 - 1], pass_send.at[n])
    wait_bytes(energy_early.at[0:len(peers)], energy_send.at[0])
    wait_bytes(energy_last.at[0:len(peers)], energy_send.at[1])


def hand_over(steps_in, energy_in, steps_out, energy_out, sems):
    copies = (
        pltpu.make_async_copy(steps_in, steps_out, sems.at[0]),
        pltpu.make_async_copy(energy_in, energy_out, sems.at[1]),
    )
    for copy in copies:
        copy.start()
    for copy in copies:
        copy.wait()


def local(
    sources,
    history,
    inverse_diagonal,
    far_cores,
    target_basis,
    source_basis,
    near_blocks,
    near_tile,
    near_count,
):
    rows, _, lags, tile, fields = history.shape
    cols, rank = far_cores.shape[1:3]
    steps = sources.shape[2]
    slots = near_blocks.shape[2]
    panel_total = rows * cols * tile
    lanes = min(128, tile, rows * rank)
    block = min(64, tile)
    dma = pltpu.SemaphoreType.DMA
    anywhere = pl.BlockSpec(memory_space=pltpu.HBM)
    inside = pl.BlockSpec(memory_space=pltpu.VMEM)
    new_steps, energies = pl.pallas_call(
        functools.partial(march, rows, cols, panel_total),
        out_shape=(
            pltpu.VMEM((steps, tile, fields), BF16),
            pltpu.VMEM((steps, fields), F32),
        ),
        in_specs=[anywhere] * 9,
        out_specs=(inside, inside),
        scratch_shapes=[
            pltpu.SMEM((1, 1, slots), jnp.int32),
            pltpu.SMEM((1, 1), jnp.int32),
            pltpu.VMEM((rows, rank, tile), BF16),
            pltpu.VMEM((rows, lags, tile, fields), BF16),
            pltpu.VMEM((cols * rank, lags * rows * rank), BF16),
            pltpu.VMEM((slots, tile, lags * tile), BF16),
            pltpu.VMEM((rank, tile), BF16),
            pltpu.VMEM((1, tile), F32),
            pltpu.VMEM((steps, tile, fields), BF16),
            pltpu.VMEM((tile, fields), F32),
            pltpu.VMEM((cols * rank, rows, lags, rank), BF16),
            pltpu.VMEM((slots, tile, lags, tile), BF16),
            pltpu.VMEM((max(tile, 2 * rows * rank) // lanes, block * lags, lanes), F32),
            pltpu.VMEM((lags, rows, rank, fields), BF16),
            tuple(pltpu.VMEM((rows, tile, fields), BF16) for _ in range(steps - 1)),
            pltpu.VMEM((steps - 1, rows, rank, fields), BF16),
            pltpu.VMEM((steps, cols, rank, fields), BF16),
            pltpu.VMEM((steps, cols, rank, fields), BF16),
            pltpu.VMEM((steps, tile, fields), F32),
            pltpu.VMEM((cols * rank, fields), F32),
            pltpu.VMEM((steps, 1, fields), F32),
            pltpu.VMEM((rows * cols, steps - 1, 1, fields), F32),
            pltpu.VMEM((rows * cols, 1, fields), F32),
            dma((8,)),
            dma(((lags + 1) // 2,)),
            dma((steps - 1,)),
            dma((steps - 1, rows // 2)),
            dma((steps - 1,)),
            dma((steps - 1,)),
            dma((steps - 1,)),
            dma((steps - 1,)),
            dma((steps,)),
            dma((steps,)),
            dma((2,)),
            dma((2,)),
        ],
        compiler_params=pltpu.CompilerParams(
            collective_id=0, has_side_effects=True, vmem_limit_bytes=58 * 1024 * 1024
        ),
    )(
        near_tile,
        near_count,
        jnp.swapaxes(source_basis[:, 0], 1, 2),
        history[:, 0],
        far_cores.reshape(cols * rank, rows, lags, rank),
        near_blocks[0, 0],
        jnp.swapaxes(target_basis[0, 0], 0, 1),
        inverse_diagonal[0],
        sources[0, 0],
    )
    new_steps, energies = pl.pallas_call(
        hand_over,
        out_shape=(
            jax.ShapeDtypeStruct((steps, tile, fields), BF16),
            jax.ShapeDtypeStruct((steps, fields), F32),
        ),
        in_specs=(inside, inside),
        out_specs=(anywhere, anywhere),
        scratch_shapes=[dma((2,))],
    )(
        pltpu.with_memory_space_constraint(new_steps, pltpu.VMEM),
        pltpu.with_memory_space_constraint(energies, pltpu.VMEM),
    )
    return new_steps[None, None], energies


def solution(mesh):
    placed = (
        P("row", "col", None, None, None),
        P(None, "col", None, None, None),
        P("row", "col", None),
        P("row", None, None, None, "col", None, None),
        P("row", "col", None, None),
        P(None, "col", None, None),
        P("row", "col", None, None, None, None),
        P("row", "col", None),
        P("row", "col"),
    )
    return jax.shard_map(
        local,
        mesh=mesh,
        in_specs=placed,
        out_specs=(P("row", "col", None, None, None), P()),
        check_vma=False,
    )
```

```python
import contextlib
import functools

import jax
import jax.numpy as jnp
from jax import lax
from jax.experimental import pallas as pl
from jax.experimental.pallas import tpu as pltpu
from jax.sharding import PartitionSpec as P

MESH = pl.DeviceIdType.MESH
F32 = jnp.float32
BF16 = jnp.bfloat16
scope = contextlib.nullcontext


def march(
    rows,
    cols,
    panel_total,
    tiles_hbm,
    count_hbm,
    basis_hbm,
    history_hbm,
    cores_hbm,
    near_hbm,
    target_hbm,
    scaling_hbm,
    sources_hbm,
    steps_ref,
    energy_ref,
    tiles_ref,
    count_ref,
    basis,
    history,
    cores,
    near_blocks,
    target,
    scaling_row,
    sources,
    scaling,
    cores_raw,
    near_raw,
    stage,
    past_proj,
    lifts,
    mixer,
    hub_cores,
    lead,
    older_out,
    older_in,
    first_out,
    first_in,
    sums_out,
    sums_in,
    sums_base,
    pairs,
    drive,
    plane_proj,
    drive_tiles,
    fresh_tiles,
    near_sum,
    energy_own,
    energy_early,
    energy_last,
    load_sems,
    history_sems,
    start_send,
    start_recv,
    older_send,
    older_recv,
    drive_send,
    drive_recv,
    plane_send,
    plane_recv,
    pair_send,
    pair_recv,
    sums_send,
    sums_recv,
    tile_send,
    tile_recv,
    pass_send,
    pass_recv,
    energy_send,
    energy_recv,
):
    step_count = sources.shape[0]
    lag_count, _, rank, fields = past_proj.shape
    tile = history.shape[2]
    slot_count = near_blocks.shape[0]
    width = rows * rank
    chips = rows // 2
    depths = cols // 2
    my_row = lax.axis_index("row")
    my_col = lax.axis_index("col")
    side = lax.rem(my_row, 2)
    chip = my_row // 2
    my_z = my_col // 2
    my_x = lax.rem(my_col, 2)
    partner = my_row + 1 - 2 * side
    hub_row = 2 * chip + 1
    is_hub = side == 1
    own_pair = pl.ds(2 * chip, 2)
    plane_pair = pl.ds(my_x * rows + 2 * chip, 2)
    me = my_row * cols + my_col

    def row_peer(d):
        return lax.rem(my_row + d, rows)

    def col_peer(d):
        return lax.rem(my_col + d, cols)

    def far_depth(i):
        up = i + (i - my_z + depths) // depths
        mirrored = depths - 1 - my_z
        down = depths - 1 - (i + (i - mirrored + depths) // depths)
        upper = 2 * my_z // depths
        return upper * up + (1 - upper) * down

    loads = [
        pltpu.make_async_copy(src, dst, load_sems.at[n])
        for n, (src, dst) in enumerate(
            (
                (basis_hbm, basis),
                (cores_hbm, cores_raw),
                (near_hbm, near_raw),
                (target_hbm, target),
                (scaling_hbm, scaling_row),
                (sources_hbm, sources),
                (tiles_hbm, tiles_ref),
                (count_hbm, count_ref),
            )
        )
    ]
    spans = [(lag, min(2, lag_count - lag)) for lag in range(0, lag_count, 2)]

    def history_load(index):
        first, length = spans[index]
        return pltpu.make_async_copy(
            history_hbm.at[:, first:first + length],
            history.at[:, first:first + length],
            history_sems.at[index],
        )

    def wait_bytes(ref, sem):
        pltpu.make_async_copy(ref, ref, sem).wait()

    for load in (loads[1], loads[0], *loads[3:5]):
        load.start()
    for index in range(len(spans)):
        history_load(index).start()

    barrier = pltpu.get_barrier_semaphore()
    peers = [(a, b) for a in range(rows) for b in range(cols) if a or b]

    def greet(index, carry):
        pl.semaphore_signal(
            barrier, inc=1, device_id=(row_peer(index // cols), col_peer(lax.rem(index, cols))),
            device_id_type=MESH,
        )
        return carry

    lax.fori_loop(1, rows * cols, greet, 0)

    def copy_to(src, dst, send, recv, row, col):
        return pltpu.make_async_remote_copy(
            src_ref=src, dst_ref=dst, send_sem=send, recv_sem=recv,
            device_id=(row, col), device_id_type=MESH,
        )

    def first_copy(z, x):
        return copy_to(
            first_out.at[x, z], first_in.at[side * cols + my_col],
            start_send.at[0], start_recv.at[0], hub_row, z * 2 + x,
        )

    def cores_copies(x, later):
        return [
            copy_to(
                cores.at[x, :, k * width:(k + 1) * width], hub_cores.at[my_x * 2 + side, k],
                start_send.at[1 + 2 * later], start_recv.at[1 + 2 * later],
                hub_row, my_z * 2 + x,
            )
            for k in (range(1, step_count - 1) if later else (0,))
        ]

    def lift_copy(d):
        return copy_to(
            lifts.at[my_row], lifts.at[my_row],
            start_send.at[2], start_recv.at[2], row_peer(d), my_col,
        )

    def older_copy(n, x):
        return copy_to(
            older_out.at[n - 1, x], older_in.at[n - 1, my_x * 2 + side],
            older_send.at[0], older_recv.at[n - 1], hub_row, my_z * 2 + x,
        )

    def drive_copy(n):
        return copy_to(
            drive.at[n, 0], drive.at[n, 0], drive_send.at[0], drive_recv.at[n], hub_row, my_col
        )

    def plane_copy(n, dy, dx):
        return copy_to(
            plane_proj.at[n, plane_pair], plane_proj.at[n, plane_pair],
            plane_send.at[0], plane_recv.at[n],
            2 * lax.rem(chip + dy, chips) + 1, my_z * 2 + lax.rem(my_x + dx, 2),
        )

    def pair_copy(n, d):
        return copy_to(
            pairs.at[n, own_pair], pairs.at[n, own_pair],
            pair_send.at[0], pair_recv.at[n], row_peer(d), my_col,
        )

    def sums_copy(n, z):
        return copy_to(
            sums_out.at[n - 1, z], sums_in.at[n - 1, my_z],
            sums_send.at[0], sums_recv.at[n - 1], my_row, z * 2 + my_x,
        )

    def last_copy(z, c):
        return copy_to(
            sums_out.at[step_count - 2, z, c], sums_in.at[step_count - 2, my_z, c],
            sums_send.at[1], sums_recv.at[step_count - 2], hub_row - 1 + c, z * 2 + my_x,
        )

    def tile_copy(n, part, owner, to):
        return copy_to(
            drive_tiles.at[n, part, owner], drive_tiles.at[n, part, owner],
            tile_send.at[0], tile_recv.at[n, part, owner // 2], to, my_col,
        )

    def pass_copy(n, part, owner):
        return copy_to(
            drive_tiles.at[n, part, owner], drive_tiles.at[n, part, owner],
            pass_send.at[0], pass_recv.at[n, part], partner, my_col,
        )

    def energy_copy(last, d):
        return copy_to(
            energy_own.at[step_count - 1] if last else energy_own.at[0:step_count - 1],
            energy_last.at[me] if last else energy_early.at[me],
            energy_send.at[last], energy_recv.at[last],
            row_peer(peers[d][0]), col_peer(peers[d][1]),
        )

    plane_peers = [(dy, dx) for dy in reversed(range(chips)) for dx in (1, 0) if dy or dx]

    def far_sum(n, x):
        depth = lag_count - n
        return jnp.dot(
            cores[x, :, n * width:],
            past_proj[0:depth].reshape(depth * width, fields),
            preferred_element_type=F32,
        ).astype(BF16)

    def near_base(n):
        depth = lag_count - n

        def add_slot(slot, carry):
            where = tiles_ref[0, 0, slot]
            value = jnp.dot(
                near_blocks[slot, :, n * tile:],
                history[where, 0:depth].reshape(depth * tile, fields),
                preferred_element_type=F32,
            )
            for lag in range(1, n):
                value += jnp.dot(
                    near_blocks[slot, :, lag * tile:(lag + 1) * tile],
                    fresh_tiles[n - 1 - lag][where],
                    preferred_element_type=F32,
                )
            near_sum[n] += value
            return carry

        near_sum[n] = jnp.zeros((tile, fields), F32)
        lax.fori_loop(0, slot_count, add_slot, 0)

    half = fields // 2

    def near_finish(n, parts):
        here = slice(parts[0] * half, (parts[-1] + 1) * half)
        total = near_sum[n, :, here]
        if n:
            for slot in range(slot_count):
                total += jnp.dot(
                    near_blocks[slot, :, 0:tile],
                    fresh_tiles[n - 1][tiles_ref[0, 0, slot], :, here],
                    preferred_element_type=F32,
                )
        driven = scaling[:, here] * (sources[n, :, here].astype(F32) - total)
        near_sum[n, :, here] = driven
        if n + 1 < step_count:
            sent = driven.astype(BF16)
            for part in parts:
                first = (part - parts[0]) * half
                drive_tiles[n, part, my_row] = sent[:, first:first + half]
                for d in range(2, rows, 2):
                    tile_copy(n, part, my_row, row_peer(d)).start()
                tile_copy(n, part, my_row, partner).start()
            drive[n, side, :, here] = jnp.dot(
                basis[my_row], sent, preferred_element_type=F32
            )
            if parts[-1] == 1:

                @pl.when(side == 0)
                def _():
                    drive_copy(n).start()

    def tiles_land(n, part):
        for d in range(2, rows, 2):
            tile_copy(n, part, row_peer(d), partner).wait_recv()
            pass_copy(n, part, row_peer(d)).start()

    def tiles_close(n, part):
        tile_copy(n, part, partner, partner).wait_recv()
        wait_bytes(drive_tiles.at[n, part, 0:chips - 1], pass_recv.at[n, part])

    def settle(n):
        far = lax.dot_general(
            target[...], pairs[n, my_row], (((0,), (0,)), ((), ())), preferred_element_type=F32
        )
        fresh = (near_sum[n] - scaling[...] * far).astype(BF16)
        steps_ref[n] = fresh
        if n + 1 < step_count:
            fresh_tiles[n][my_row] = fresh

    def rebuild(n, part):
        here = slice(part * half, (part + 1) * half)
        for d in range(1, rows):
            p = row_peer(d)
            far = lax.dot_general(
                lifts[p], pairs[n, p, :, here], (((0,), (0,)), ((), ())),
                preferred_element_type=F32,
            )
            fresh_tiles[n][p, :, here] = (drive_tiles[n, part, p].astype(F32) - far).astype(BF16)

    def measure_energy(n):
        energy_own[n] = (
            jnp.sum(jnp.square(steps_ref[n].astype(F32)), axis=0, keepdims=True) / panel_total
        )

    def publish(n, core):
        mine = core.astype(BF16)
        pairs[n, own_pair] = mine
        wait_bytes(drive.at[n, 0], drive_recv.at[n])
        mixed = jnp.dot(
            mixer[...], mine.reshape(2 * rank, fields), preferred_element_type=F32
        )
        plane_proj[n, plane_pair] = (
            drive[n] - mixed.reshape(2, rank, fields)
        ).astype(BF16)
        for dy, dx in plane_peers:
            plane_copy(n, dy, dx).start()
        for d in (rows - 1, *range(1, rows - 1)):
            pair_copy(n, d).start()

    lanes = stage.shape[2]
    block = stage.shape[1] // lag_count

    def spread(value, base=0):
        for c in range(value.shape[1] // lanes):
            stage[base + c, 0:value.shape[0]] = value[:, c * lanes:(c + 1) * lanes]

    def pick(lag, c, length):
        return stage[c, pl.ds(lag, length, stride=lag_count), :].astype(BF16)

    def pack_cores(z):
        span = 2 * rank
        here = pl.ds(z * span, span)
        base = z % (stage.shape[0] * lanes // width) * (width // lanes)
        total = None
        for p in range(rows):
            value = cores_raw[here, p].astype(F32).reshape(span * lag_count, rank).astype(BF16)
            place = (
                lax.broadcasted_iota(jnp.int32, (rank, width), 1)
                == lax.broadcasted_iota(jnp.int32, (rank, width), 0) + p * rank
            )
            term = jnp.dot(
                value, place.astype(F32).astype(BF16), preferred_element_type=F32
            )
            total = term if total is None else total + term
        spread(total, base)
        for lag in range(lag_count):
            for c in range(width // lanes):
                first = lag * width + c * lanes
                both = pick(lag, base + c, span)
                for x in range(2):
                    cores[x, z * rank:(z + 1) * rank, first:first + lanes] = (
                        both[x * rank:(x + 1) * rank]
                    )

    def pack_near(index, carry):
        slot = index // (tile // block)
        here = pl.ds(pl.multiple_of(lax.rem(index, tile // block) * block, block), block)
        spread(near_raw[slot, here].astype(F32).reshape(block * lag_count, tile))
        for lag in range(lag_count):
            for c in range(tile // lanes):
                first = lag * tile + c * lanes
                near_blocks[slot, here, first:first + lanes] = jnp.where(
                    slot < count_ref[0, 0], pick(lag, c, block), jnp.zeros((block, lanes), BF16)
                )
        return carry

    with scope("w_cores"):
        loads[1].wait()
        for load in (loads[2], *loads[5:]):
            load.start()
    with scope("pack_cores"):
        for z in range(depths):
            pack_cores(z)
        loads[0].wait()
    with scope("project"):
        for index, (first, length) in enumerate(spans):
            history_load(index).wait()
            for lag in range(first, first + length):
                for p in range(rows):
                    past_proj[lag, p] = jnp.dot(
                        basis[p], history[p, lag], preferred_element_type=F32
                    ).astype(BF16)

    for x in range(2):
        first_out[x] = far_sum(0, x).reshape(depths, rank, fields)
    with scope("barrier"):
        pl.semaphore_wait(barrier, rows * cols - 1)
    for i in range(depths - 1):
        for x in (1 - my_x, my_x):
            first_copy(far_depth(i), x).start()
    first_copy(my_z, 1 - my_x).start()

    @pl.when(is_hub)
    def _():
        first_in[cols + my_col] = first_out[my_x, my_z]

    @pl.when(side == 0)
    def _():
        first_copy(my_z, my_x).start()

    with scope("lifts"):
        for load in loads[3:5]:
            load.wait()
        lifts[my_row] = (target[...].astype(F32) * scaling_row[...]).astype(BF16)
        for d in range(1, rows):
            lift_copy(d).start()

    def send_older(n):
        for x in range(2):
            older_out[n - 1, x] = far_sum(n, x)
        older_copy(n, 1 - my_x).start()

        @pl.when(side == 0)
        def _():
            older_copy(n, my_x).start()

        @pl.when(is_hub)
        def _():
            older_in[n - 1, my_x * 2 + 1] = older_out[n - 1, my_x]

    def send_cores(later):
        for copy in cores_copies(1 - my_x, later):
            copy.start()

        @pl.when(side == 0)
        def _():
            for copy in cores_copies(my_x, later):
                copy.start()

        @pl.when(is_hub)
        def _():
            for k in range(1, step_count - 1) if later else (0,):
                hub_cores[my_x * 2 + 1, k] = cores[my_x, :, k * width:(k + 1) * width]

    with scope("older1"):
        send_cores(0)
        send_older(1)
    with scope("near0"):
        for load in (loads[2], *loads[6:]):
            load.wait()
        lax.fori_loop(0, slot_count * (tile // block), pack_near, 0)
        near_base(0)
        loads[5].wait()
        scaling[...] = jnp.transpose(jnp.broadcast_to(scaling_row[...], (fields, tile)))
        near_finish(0, (0, 1))
    with scope("w_lifts"):
        wait_bytes(lifts.at[0:rows - 1], start_recv.at[2])

    @pl.when(is_hub)
    def _():
        for c in range(2):
            own = lax.dot_general(
                basis[2 * chip + c], lifts[2 * chip + c], (((1,), (1,)), ((), ())),
                preferred_element_type=F32,
            ).astype(BF16)
            none = jnp.zeros((rank, rank), BF16)
            mixer[c * rank:(c + 1) * rank] = jnp.concatenate(
                [own, none] if c == 0 else [none, own], axis=1
            )
        with scope("w_first"):
            wait_bytes(first_in.at[0:2 * cols - 1], start_recv.at[0])
        core = []
        for c in range(2):
            total = first_in[c * cols].astype(F32)
            for j in range(1, cols):
                total += first_in[c * cols + j].astype(F32)
            core.append(total)
        publish(0, jnp.stack(core))

    with scope("older2"):
        send_cores(1)
        for n in range(2, step_count):
            send_older(n)

    def lead_rows(later):
        for k in range(1, step_count - 1) if later else (0,):
            for z in range(depths):
                for c in range(2):
                    for x in range(2):
                        lead[k, z * 2 + c, :, x * width:(x + 1) * width] = hub_cores[
                            x * 2 + c, k, z * rank:(z + 1) * rank
                        ]

    last = step_count - 1
    for n in range(1, step_count):
        with scope("near_base"):
            near_base(n)

        @pl.when(is_hub)
        def _():
            with scope("base"):
                if n == 1:
                    wait_bytes(hub_cores.at[0:3, 0], start_recv.at[1])
                    lead_rows(0)
                if n == 2:
                    wait_bytes(hub_cores.at[0:3, 1:], start_recv.at[3])
                    lead_rows(1)
                wait_bytes(older_in.at[n - 1, 0:3], older_recv.at[n - 1])
                for z in range(depths):
                    for c in range(2):
                        here = slice(z * rank, (z + 1) * rank)
                        sums_base[z * 2 + c] = older_in[n - 1, c, here].astype(
                            F32
                        ) + older_in[n - 1, 2 + c, here].astype(F32)
                for lag in range(1, n):
                    sums_base[...] += jnp.dot(
                        lead[lag].reshape(cols * rank, 2 * width),
                        plane_proj[n - 1 - lag].reshape(2 * width, fields),
                        preferred_element_type=F32,
                    ).reshape(cols, rank, fields)
            settle(n - 1)

        with scope("w_land0"):
            tiles_land(n - 1, 0)

        @pl.when(is_hub)
        def _():
            with scope("w_plane"):
                wait_bytes(plane_proj.at[n - 1, 0:2 * len(plane_peers)], plane_recv.at[n - 1])
            value = sums_base[...] + jnp.dot(
                lead[0].reshape(cols * rank, 2 * width),
                plane_proj[n - 1].reshape(2 * width, fields),
                preferred_element_type=F32,
            ).reshape(cols, rank, fields)
            sums_out[n - 1] = value.astype(BF16).reshape(depths, 2, rank, fields)
            for i in range(depths - 1):
                if n < last:
                    sums_copy(n, far_depth(i)).start()
                else:
                    last_copy(far_depth(i), 0).start()
                    last_copy(far_depth(i), 1).start()
            if n == last:
                last_copy(my_z, 0).start()
            sums_in[n - 1, my_z] = sums_out[n - 1, my_z]
            wait_bytes(pairs.at[n - 1, 0:2 * (chips - 1)], pair_recv.at[n - 1])

        with scope("w_tiles0"):
            tiles_close(n - 1, 0)

        @pl.when(side == 0)
        def _():
            with scope("w_pairs"):
                wait_bytes(pairs.at[n - 1], pair_recv.at[n - 1])
            settle(n - 1)

        with scope("w_tiles1"):
            tiles_land(n - 1, 1)
        with scope("finish0"):
            rebuild(n - 1, 0)
            if n + 1 < step_count:
                near_finish(n, (0,))
        with scope("w_tiles2"):
            tiles_close(n - 1, 1)
        with scope("finish1"):
            rebuild(n - 1, 1)
            near_finish(n, (1,) if n + 1 < step_count else (0, 1))
        measure_energy(n - 1)
        if n + 1 == step_count:
            for d in range(len(peers)):
                energy_copy(0, d).start()

        if n < last:

            @pl.when(is_hub)
            def _():
                with scope("w_sums"):
                    wait_bytes(sums_in.at[n - 1, 0:depths - 1], sums_recv.at[n - 1])
                total = sums_in[n - 1, 0].astype(F32)
                for z in range(1, depths):
                    total += sums_in[n - 1, z].astype(F32)
                publish(n, total)

    @pl.when(side == 0)
    def _():
        with scope("w_last"):
            wait_bytes(first_in.at[0:depths], sums_recv.at[last - 1])

    @pl.when(is_hub)
    def _():
        with scope("w_last"):
            wait_bytes(first_in.at[0:depths - 1], sums_recv.at[last - 1])

    total = sums_in[last - 1, 0, side].astype(F32)
    for z in range(1, depths):
        total += sums_in[last - 1, z, side].astype(F32)
    pairs[last, my_row] = total.astype(BF16)
    settle(last)
    measure_energy(last)
    for d in range(len(peers)):
        energy_copy(1, d).start()
    energy_early[me] = energy_own[0:last]
    energy_last[me] = energy_own[last]
    for group, where in ((0, energy_early), (1, energy_last)):
        with scope("w_energy"):
            wait_bytes(where.at[0:len(peers)], energy_recv.at[group])
        total = where[0]
        for origin in range(1, rows * cols):
            total += where[origin]
        if group:
            energy_ref[last:last + 1, :] = total
        else:
            for n in range(last):
                energy_ref[n:n + 1, :] = total[n]

    with scope("w_sends"):
        wait_bytes(lifts.at[0:rows - 1], start_send.at[2])
        wait_bytes(drive_tiles.at[:, :, 0:chips], tile_send.at[0])
        wait_bytes(drive_tiles.at[:, :, 0:chips - 1], pass_send.at[0])
        wait_bytes(energy_early.at[0:len(peers)], energy_send.at[0])
        wait_bytes(energy_last.at[0:len(peers)], energy_send.at[1])

        @pl.when(side == 0)
        def _():
            wait_bytes(first_in.at[0:cols], start_send.at[0])
            wait_bytes(hub_cores.at[0:2, 0], start_send.at[1])
            wait_bytes(hub_cores.at[0:2, 1:], start_send.at[3])
            wait_bytes(older_in.at[:, 0:2], older_send.at[0])
            wait_bytes(drive.at[:, 0], drive_send.at[0])

        @pl.when(is_hub)
        def _():
            wait_bytes(first_in.at[0:cols - 1], start_send.at[0])
            wait_bytes(hub_cores.at[0:1, 0], start_send.at[1])
            wait_bytes(hub_cores.at[0:1, 1:], start_send.at[3])
            wait_bytes(older_in.at[:, 0:1], older_send.at[0])
            wait_bytes(plane_proj.at[:, 0:2 * len(plane_peers)], plane_send.at[0])
            wait_bytes(plane_proj.at[:, 0:2 * (rows - 1)], pair_send.at[0])
            wait_bytes(sums_in.at[0:last - 1, 0:depths - 1], sums_send.at[0])
            wait_bytes(first_in.at[0:2 * depths - 1], sums_send.at[1])


def hand_over(steps_in, energy_in, steps_out, energy_out, sems):
    copies = (
        pltpu.make_async_copy(steps_in, steps_out, sems.at[0]),
        pltpu.make_async_copy(energy_in, energy_out, sems.at[1]),
    )
    for copy in copies:
        copy.start()
    for copy in copies:
        copy.wait()


def local(
    sources,
    history,
    inverse_diagonal,
    far_cores,
    target_basis,
    source_basis,
    near_blocks,
    near_tile,
    near_count,
):
    rows, _, lags, tile, fields = history.shape
    cols, rank = far_cores.shape[1:3]
    steps = sources.shape[2]
    slots = near_blocks.shape[2]
    panel_total = rows * cols * tile
    width = rows * rank
    depths = cols // 2
    lanes = min(128, tile, width)
    block = min(64, tile)
    dma = pltpu.SemaphoreType.DMA
    anywhere = pl.BlockSpec(memory_space=pltpu.HBM)
    inside = pl.BlockSpec(memory_space=pltpu.VMEM)
    new_steps, energies = pl.pallas_call(
        functools.partial(march, rows, cols, panel_total),
        out_shape=(
            pltpu.VMEM((steps, tile, fields), BF16),
            pltpu.VMEM((steps, fields), F32),
        ),
        in_specs=[anywhere] * 9,
        out_specs=(inside, inside),
        scratch_shapes=[
            pltpu.SMEM((1, 1, slots), jnp.int32),
            pltpu.SMEM((1, 1), jnp.int32),
            pltpu.VMEM((rows, rank, tile), BF16),
            pltpu.VMEM((rows, lags, tile, fields), BF16),
            pltpu.VMEM((2, depths * rank, lags * width), BF16),
            pltpu.VMEM((slots, tile, lags * tile), BF16),
            pltpu.VMEM((rank, tile), BF16),
            pltpu.VMEM((1, tile), F32),
            pltpu.VMEM((steps, tile, fields), BF16),
            pltpu.VMEM((tile, fields), F32),
            pltpu.VMEM((cols * rank, rows, lags, rank), BF16),
            pltpu.VMEM((slots, tile, lags, tile), BF16),
            pltpu.VMEM((max(tile, width) // lanes, block * lags, lanes), F32),
            pltpu.VMEM((lags, rows, rank, fields), BF16),
            pltpu.VMEM((rows, rank, tile), BF16),
            pltpu.VMEM((2 * rank, 2 * rank), BF16),
            pltpu.VMEM((4, steps - 1, depths * rank, width), BF16),
            pltpu.VMEM((steps - 1, cols, rank, 2 * width), BF16),
            pltpu.VMEM((steps - 1, 2, depths * rank, fields), BF16),
            pltpu.VMEM((steps - 1, 4, depths * rank, fields), BF16),
            pltpu.VMEM((2, depths, rank, fields), BF16),
            pltpu.VMEM((2 * cols, rank, fields), BF16),
            pltpu.VMEM((steps - 1, depths, 2, rank, fields), BF16),
            pltpu.VMEM((steps - 1, depths, 2, rank, fields), BF16),
            pltpu.VMEM((cols, rank, fields), F32),
            pltpu.VMEM((steps, rows, rank, fields), BF16),
            pltpu.VMEM((steps - 1, 2, rank, fields), F32),
            pltpu.VMEM((steps - 1, 2 * rows, rank, fields), BF16),
            pltpu.VMEM((steps - 1, 2, rows, tile, fields // 2), BF16),
            tuple(pltpu.VMEM((rows, tile, fields), BF16) for _ in range(steps - 1)),
            pltpu.VMEM((steps, tile, fields), F32),
            pltpu.VMEM((steps, 1, fields), F32),
            pltpu.VMEM((rows * cols, steps - 1, 1, fields), F32),
            pltpu.VMEM((rows * cols, 1, fields), F32),
            dma((8,)),
            dma(((lags + 1) // 2,)),
            dma((4,)),
            dma((4,)),
            dma((1,)),
            dma((steps - 1,)),
            dma((1,)),
            dma((steps - 1,)),
            dma((1,)),
            dma((steps - 1,)),
            dma((1,)),
            dma((steps - 1,)),
            dma((2,)),
            dma((steps - 1,)),
            dma((1,)),
            dma((steps - 1, 2, rows // 2)),
            dma((1,)),
            dma((steps - 1, 2)),
            dma((2,)),
            dma((2,)),
        ],
        compiler_params=pltpu.CompilerParams(
            collective_id=0, has_side_effects=True, vmem_limit_bytes=63 * 1024 * 1024
        ),
    )(
        near_tile,
        near_count,
        jnp.swapaxes(source_basis[:, 0], 1, 2),
        history[:, 0],
        far_cores.reshape(cols * rank, rows, lags, rank),
        near_blocks[0, 0],
        jnp.swapaxes(target_basis[0, 0], 0, 1),
        inverse_diagonal[0],
        sources[0, 0],
    )
    new_steps, energies = pl.pallas_call(
        hand_over,
        out_shape=(
            jax.ShapeDtypeStruct((steps, tile, fields), BF16),
            jax.ShapeDtypeStruct((steps, fields), F32),
        ),
        in_specs=(inside, inside),
        out_specs=(anywhere, anywhere),
        scratch_shapes=[dma((2,))],
    )(
        pltpu.with_memory_space_constraint(new_steps, pltpu.VMEM),
        pltpu.with_memory_space_constraint(energies, pltpu.VMEM),
    )
    return new_steps[None, None], energies


def solution(mesh):
    placed = (
        P("row", "col", None, None, None),
        P(None, "col", None, None, None),
        P("row", "col", None),
        P("row", None, None, None, "col", None, None),
        P("row", "col", None, None),
        P(None, "col", None, None),
        P("row", "col", None, None, None, None),
        P("row", "col", None),
        P("row", "col"),
    )
    return jax.shard_map(
        local,
        mesh=mesh,
        in_specs=placed,
        out_specs=(P("row", "col", None, None, None), P()),
        check_vma=False,
    )
```

```python
import contextlib
import functools

import jax
import jax.numpy as jnp
from jax import lax
from jax.experimental import pallas as pl
from jax.experimental.pallas import tpu as pltpu
from jax.sharding import PartitionSpec as P

MESH = pl.DeviceIdType.MESH
F32 = jnp.float32
BF16 = jnp.bfloat16
scope = contextlib.nullcontext


def march(
    rows,
    cols,
    panel_total,
    tiles_hbm,
    count_hbm,
    basis_hbm,
    history_hbm,
    cores_hbm,
    near_hbm,
    target_hbm,
    scaling_hbm,
    sources_hbm,
    steps_ref,
    energy_ref,
    tiles_ref,
    count_ref,
    basis,
    history,
    cores,
    near_blocks,
    target,
    scaling_row,
    sources,
    scaling,
    cores_raw,
    near_raw,
    stage,
    past_proj,
    lifts,
    weave,
    mixer,
    hub_cores,
    lead,
    older_out,
    older_in,
    first_out,
    first_in,
    sums_out,
    sums_in,
    sums_base,
    pairs,
    drive,
    plane_proj,
    drive_tiles,
    tile_pool,
    core_pool,
    fresh_tiles,
    near_sum,
    energy_own,
    energy_early,
    energy_last,
    load_sems,
    history_sems,
    send_sems,
    start_recv,
    cores_recv,
    older_recv,
    drive_recv,
    plane_recv,
    pair_recv,
    sums_recv,
    tile_recv,
    pass_recv,
    energy_recv,
):
    step_count = sources.shape[0]
    lag_count, _, rank, fields = past_proj.shape
    tile = history.shape[2]
    slot_count = near_blocks.shape[0]
    width = rows * rank
    chips = rows // 2
    depths = cols // 2
    my_row = lax.axis_index("row")
    my_col = lax.axis_index("col")
    side = lax.rem(my_row, 2)
    chip = my_row // 2
    my_z = my_col // 2
    my_x = lax.rem(my_col, 2)
    partner = my_row + 1 - 2 * side
    hub_row = 2 * chip + 1
    is_hub = side == 1
    own_pair = pl.ds(2 * chip, 2)
    plane_pair = pl.ds(my_x * rows + 2 * chip, 2)
    me = my_row * cols + my_col

    def row_peer(d):
        return lax.rem(my_row + d, rows)

    def col_peer(d):
        return lax.rem(my_col + d, cols)

    def far_depth(i):
        up = i + (i - my_z + depths) // depths
        mirrored = depths - 1 - my_z
        down = depths - 1 - (i + (i - mirrored + depths) // depths)
        upper = 2 * my_z // depths
        return upper * up + (1 - upper) * down

    loads = [
        pltpu.make_async_copy(src, dst, load_sems.at[n])
        for n, (src, dst) in enumerate(
            (
                (basis_hbm, basis),
                (cores_hbm, cores_raw),
                (near_hbm, near_raw),
                (target_hbm, target),
                (scaling_hbm, scaling_row),
                (sources_hbm, sources),
                (tiles_hbm, tiles_ref),
                (count_hbm, count_ref),
            )
        )
    ]
    spans = [(lag, min(2, lag_count - lag)) for lag in range(0, lag_count, 2)]

    def history_load(index):
        first, length = spans[index]
        return pltpu.make_async_copy(
            history_hbm.at[:, first:first + length],
            history.at[:, first:first + length],
            history_sems.at[index],
        )

    def wait_bytes(ref, sem):
        pltpu.make_async_copy(ref, ref, sem).wait()

    for load in (loads[1], loads[0], *loads[3:5]):
        load.start()
    for index in range(len(spans)):
        history_load(index).start()

    barrier = pltpu.get_barrier_semaphore()
    peers = [(a, b) for a in range(rows) for b in range(cols) if a or b]

    def greet(index, carry):
        pl.semaphore_signal(
            barrier, inc=1, device_id=(row_peer(index // cols), col_peer(lax.rem(index, cols))),
            device_id_type=MESH,
        )
        return carry

    lax.fori_loop(1, rows * cols, greet, 0)

    def copy_to(src, dst, send, recv, row, col):
        return pltpu.make_async_remote_copy(
            src_ref=src, dst_ref=dst, send_sem=send, recv_sem=recv,
            device_id=(row, col), device_id_type=MESH,
        )

    def first_copy(z, x):
        return copy_to(
            first_out.at[x, z], first_in.at[side * cols + my_col],
            load_sems.at[0], start_recv.at[0], hub_row, z * 2 + x,
        )

    def cores_copy(k, x):
        return copy_to(
            cores.at[x, :, k * width:(k + 1) * width], hub_cores.at[my_x * 2 + side, k],
            load_sems.at[3], cores_recv.at[k], hub_row, my_z * 2 + x,
        )

    def lift_copy(d):
        return copy_to(
            lifts.at[my_row], lifts.at[my_row],
            load_sems.at[1], start_recv.at[1], row_peer(d), my_col,
        )

    def older_copy(n, x):
        return copy_to(
            older_out.at[n - 1, x], older_in.at[n - 1, my_x * 2 + side],
            load_sems.at[4], older_recv.at[n - 1], hub_row, my_z * 2 + x,
        )

    def drive_copy(n):
        return copy_to(
            drive.at[n, 0], drive.at[n, 0], load_sems.at[2], drive_recv.at[n], hub_row, my_col
        )

    def plane_copy(n, dy, dx):
        return copy_to(
            plane_proj.at[n, plane_pair], plane_proj.at[n, plane_pair],
            load_sems.at[5], plane_recv.at[n],
            2 * lax.rem(chip + dy, chips) + 1, my_z * 2 + lax.rem(my_x + dx, 2),
        )

    def pair_copy(n, d):
        return copy_to(
            pairs.at[n, own_pair], pairs.at[n, own_pair],
            load_sems.at[6], pair_recv.at[n], row_peer(d), my_col,
        )

    def sums_copy(n, z):
        return copy_to(
            sums_out.at[n - 1, z], sums_in.at[n - 1, my_z],
            send_sems.at[2], sums_recv.at[n - 1], my_row, z * 2 + my_x,
        )

    def last_copy(z, c):
        return copy_to(
            sums_out.at[step_count - 2, z, c], sums_in.at[step_count - 2, my_z, c],
            load_sems.at[7], sums_recv.at[step_count - 2], hub_row - 1 + c, z * 2 + my_x,
        )

    def tile_copy(n, part, owner, to, index):
        return copy_to(
            drive_tiles.at[n, part, owner], drive_tiles.at[n, part, owner],
            history_sems.at[0],
            pass_recv.at[n, part] if index is None else tile_recv.at[n, part, index],
            to, my_col,
        )

    def pass_copy(n, part, owner):
        return copy_to(
            drive_tiles.at[n, part, owner], drive_tiles.at[n, part, owner],
            history_sems.at[1], pass_recv.at[n, part], partner, my_col,
        )

    def energy_copy(last, d):
        return copy_to(
            energy_own.at[step_count - 1] if last else energy_own.at[0:step_count - 1],
            energy_last.at[me] if last else energy_early.at[me],
            send_sems.at[last], energy_recv.at[last],
            row_peer(peers[d][0]), col_peer(peers[d][1]),
        )

    plane_peers = [(dy, dx) for dy in reversed(range(chips)) for dx in (1, 0) if dy or dx]

    def far_sum(n, x):
        depth = lag_count - n
        return jnp.dot(
            cores[x, :, n * width:],
            past_proj[0:depth].reshape(depth * width, fields),
            preferred_element_type=F32,
        ).astype(BF16)

    def near_base(n):
        depth = lag_count - n

        def add_slot(slot, carry):
            where = tiles_ref[0, 0, slot]
            value = jnp.dot(
                near_blocks[slot, :, n * tile:],
                history[where, 0:depth].reshape(depth * tile, fields),
                preferred_element_type=F32,
            )
            for lag in range(1, n):
                value += jnp.dot(
                    near_blocks[slot, :, lag * tile:(lag + 1) * tile],
                    fresh_tiles[n - 1 - lag][where],
                    preferred_element_type=F32,
                )
            near_sum[n] += value
            return carry

        near_sum[n] = jnp.zeros((tile, fields), F32)
        lax.fori_loop(0, slot_count, add_slot, 0)

    half = fields // 2

    def send_tiles(n, part):
        for d in range(2, rows, 2):
            tile_copy(n, part, my_row, row_peer(d), (rows - d) // 2 - 1).start()

    def near_tiles(n, part):
        here = slice(part * half, (part + 1) * half)
        tile_pool[...] = drive_tiles[n - 1, part]
        total = near_sum[n, :, here]
        for slot in range(slot_count):
            total += jnp.dot(
                near_blocks[slot, :, 0:tile],
                tile_pool[tiles_ref[0, 0, slot]],
                preferred_element_type=F32,
            )
        near_sum[n, :, here] = total

    def near_first():
        driven = scaling[...] * (sources[0].astype(F32) - near_sum[0])
        near_sum[0] = driven
        sent = driven.astype(BF16)
        drive[0, side] = jnp.dot(basis[my_row], sent, preferred_element_type=F32)

        @pl.when(side == 0)
        def _():
            drive_copy(0).start()

        for part in range(2):
            drive_tiles[0, part, my_row] = sent[:, part * half:(part + 1) * half]
        send_tiles(0, 0)

        @pl.when(side == 0)
        def _():
            send_tiles(0, 1)

        for part in range(2):
            tile_copy(0, part, my_row, partner, None).start()

    def near_finish(n, part):
        here = slice(part * half, (part + 1) * half)
        core_pool[...] = pairs[n - 1, :, :, here]
        known = [core_pool[tiles_ref[0, 0, slot]] for slot in range(slot_count)]
        total = near_sum[n, :, here] - jnp.dot(
            weave[...], jnp.concatenate(known, axis=0), preferred_element_type=F32
        )
        driven = scaling[:, here] * (sources[n, :, here].astype(F32) - total)
        near_sum[n, :, here] = driven
        if n + 1 < step_count:
            sent = driven.astype(BF16)
            drive_tiles[n, part, my_row] = sent
            if part == 0:
                send_tiles(n, part)
            else:

                @pl.when(side == 0)
                def _():
                    send_tiles(n, part)

            tile_copy(n, part, my_row, partner, None).start()
            drive[n, side, :, here] = jnp.dot(
                basis[my_row], sent, preferred_element_type=F32
            )
            if part == 1:

                @pl.when(side == 0)
                def _():
                    drive_copy(n).start()

    def tiles_land(n, part):
        for d in range(2, rows, 2):
            tile_copy(n, part, row_peer(d), partner, d // 2 - 1).wait_recv()
            pass_copy(n, part, row_peer(d)).start()

    def tiles_close(n, part):
        wait_bytes(drive_tiles.at[n, part, 0:chips], pass_recv.at[n, part])

    def settle(n):
        far = lax.dot_general(
            target[...], pairs[n, my_row], (((0,), (0,)), ((), ())), preferred_element_type=F32
        )
        fresh = (near_sum[n] - scaling[...] * far).astype(BF16)
        energy_own[n] = (
            jnp.sum(jnp.square(fresh.astype(F32)), axis=0, keepdims=True) / panel_total
        )
        steps_ref[n] = fresh
        if n + 1 < step_count:
            fresh_tiles[n][my_row] = fresh

    def rebuild(n):
        for d in range(1, rows):
            p = row_peer(d)
            far = lax.dot_general(
                lifts[p], pairs[n, p], (((0,), (0,)), ((), ())), preferred_element_type=F32
            )
            for part in range(2):
                here = slice(part * half, (part + 1) * half)
                fresh_tiles[n][p, :, here] = (
                    drive_tiles[n, part, p].astype(F32) - far[:, here]
                ).astype(BF16)

    def publish(n, core):
        mine = core.astype(BF16)
        pairs[n, own_pair] = mine
        wait_bytes(drive.at[n, 0], drive_recv.at[n])
        mixed = jnp.dot(
            mixer[...], mine.reshape(2 * rank, fields), preferred_element_type=F32
        )
        plane_proj[n, plane_pair] = (
            drive[n] - mixed.reshape(2, rank, fields)
        ).astype(BF16)
        for dy, dx in plane_peers:
            plane_copy(n, dy, dx).start()
        for d in (rows - 1, *range(1, rows - 1, 2)):
            pair_copy(n, d).start()
        send_tiles(n, 1)
        for d in range(2, rows - 1, 2):
            pair_copy(n, d).start()

    lanes = stage.shape[2]
    block = stage.shape[1] // lag_count

    def spread(value, base=0):
        for c in range(value.shape[1] // lanes):
            stage[base + c, 0:value.shape[0]] = value[:, c * lanes:(c + 1) * lanes]

    def pick(lag, c, length):
        return stage[c, pl.ds(lag, length, stride=lag_count), :].astype(BF16)

    def pack_cores(z):
        span = 2 * rank
        here = pl.ds(z * span, span)
        base = z % (stage.shape[0] * lanes // width) * (width // lanes)
        total = None
        for p in range(rows):
            value = cores_raw[here, p].astype(F32).reshape(span * lag_count, rank).astype(BF16)
            place = (
                lax.broadcasted_iota(jnp.int32, (rank, width), 1)
                == lax.broadcasted_iota(jnp.int32, (rank, width), 0) + p * rank
            )
            term = jnp.dot(
                value, place.astype(F32).astype(BF16), preferred_element_type=F32
            )
            total = term if total is None else total + term
        spread(total, base)
        for lag in range(lag_count):
            for c in range(width // lanes):
                first = lag * width + c * lanes
                both = pick(lag, base + c, span)
                for x in range(2):
                    cores[x, z * rank:(z + 1) * rank, first:first + lanes] = (
                        both[x * rank:(x + 1) * rank]
                    )

    def pack_block(index, base):
        slot = index // (tile // block)
        here = pl.ds(pl.multiple_of(lax.rem(index, tile // block) * block, block), block)
        spread(near_raw[slot, here].astype(F32).reshape(block * lag_count, tile), base)
        for lag in range(lag_count):
            for c in range(tile // lanes):
                first = lag * tile + c * lanes
                near_blocks[slot, here, first:first + lanes] = jnp.where(
                    slot < count_ref[0, 0], pick(lag, base + c, block), jnp.zeros((block, lanes), BF16)
                )

    turns = stage.shape[0] * lanes // tile

    def pack_near(index, carry):
        for turn in range(turns):
            pack_block(index * turns + turn, turn * (tile // lanes))
        return carry

    with scope("w_cores"):
        loads[1].wait()
        for load in (loads[2], *loads[5:]):
            load.start()
    with scope("pack_cores"):
        for z in range(depths):
            pack_cores(z)
        loads[0].wait()
    with scope("project"):
        for index, (first, length) in enumerate(spans):
            history_load(index).wait()
            for lag in range(first, first + length):
                for p in range(rows):
                    past_proj[lag, p] = jnp.dot(
                        basis[p], history[p, lag], preferred_element_type=F32
                    ).astype(BF16)

    for x in range(2):
        first_out[x] = far_sum(0, x).reshape(depths, rank, fields)
    with scope("barrier"):
        pl.semaphore_wait(barrier, rows * cols - 1)
    for i in range(depths - 1):
        for x in (1 - my_x, my_x):
            first_copy(far_depth(i), x).start()
    first_copy(my_z, 1 - my_x).start()

    @pl.when(is_hub)
    def _():
        first_in[cols + my_col] = first_out[my_x, my_z]

    @pl.when(side == 0)
    def _():
        first_copy(my_z, my_x).start()

    for load in loads[3:5]:
        load.wait()
    lifts[my_row] = (target[...].astype(F32) * scaling_row[...]).astype(BF16)
    for d in range(1, rows):
        lift_copy(d).start()

    def send_older(n):
        for x in range(2):
            older_out[n - 1, x] = far_sum(n, x)
        older_copy(n, 1 - my_x).start()

        @pl.when(side == 0)
        def _():
            older_copy(n, my_x).start()

        @pl.when(is_hub)
        def _():
            older_in[n - 1, my_x * 2 + 1] = older_out[n - 1, my_x]

    def send_cores(k):
        cores_copy(k, 1 - my_x).start()

        @pl.when(side == 0)
        def _():
            cores_copy(k, my_x).start()

        @pl.when(is_hub)
        def _():
            hub_cores[my_x * 2 + 1, k] = cores[my_x, :, k * width:(k + 1) * width]

    with scope("older1"):
        send_cores(0)
        send_older(1)
    with scope("pack_near"):
        for load in (loads[2], *loads[6:]):
            load.wait()
        lax.fori_loop(0, slot_count * (tile // block) // turns, pack_near, 0)
    with scope("near_base0"):
        near_base(0)
    with scope("near0"):
        loads[5].wait()
        scaling[...] = jnp.transpose(jnp.broadcast_to(scaling_row[...], (fields, tile)))
        near_first()
    with scope("w_lifts"):
        wait_bytes(lifts.at[0:rows - 1], start_recv.at[1])
    weave[...] = jnp.concatenate(
        [
            lax.dot_general(
                near_blocks[slot, :, 0:tile], lifts[tiles_ref[0, 0, slot]],
                (((1,), (1,)), ((), ())), preferred_element_type=F32,
            )
            for slot in range(slot_count)
        ],
        axis=1,
    ).astype(BF16)

    @pl.when(is_hub)
    def _():
        for c in range(2):
            own = lax.dot_general(
                basis[2 * chip + c], lifts[2 * chip + c], (((1,), (1,)), ((), ())),
                preferred_element_type=F32,
            ).astype(BF16)
            none = jnp.zeros((rank, rank), BF16)
            mixer[c * rank:(c + 1) * rank] = jnp.concatenate(
                [own, none] if c == 0 else [none, own], axis=1
            )
        with scope("w_first"):
            wait_bytes(first_in.at[0:2 * cols - 1], start_recv.at[0])
        core = []
        for c in range(2):
            total = first_in[c * cols].astype(F32)
            for j in range(1, cols):
                total += first_in[c * cols + j].astype(F32)
            core.append(total)
        publish(0, jnp.stack(core))

    def lead_rows(k):
        for z in range(depths):
            for c in range(2):
                for x in range(2):
                    lead[k, z * 2 + c, :, x * width:(x + 1) * width] = hub_cores[
                        x * 2 + c, k, z * rank:(z + 1) * rank
                    ]

    last = step_count - 1
    for n in range(1, step_count):
        if n > 1:
            with scope("settle"):
                settle(n - 2)
                rebuild(n - 2)
        with scope("near_base"):
            near_base(n)

        @pl.when(is_hub)
        def _():
            with scope("base"):
                wait_bytes(hub_cores.at[0:3, n - 1], cores_recv.at[n - 1])
                lead_rows(n - 1)
                wait_bytes(older_in.at[n - 1, 0:3], older_recv.at[n - 1])
                for z in range(depths):
                    for c in range(2):
                        here = slice(z * rank, (z + 1) * rank)
                        sums_base[z * 2 + c] = older_in[n - 1, c, here].astype(
                            F32
                        ) + older_in[n - 1, 2 + c, here].astype(F32)
                for lag in range(1, n):
                    sums_base[...] += jnp.dot(
                        lead[lag].reshape(cols * rank, 2 * width),
                        plane_proj[n - 1 - lag].reshape(2 * width, fields),
                        preferred_element_type=F32,
                    ).reshape(cols, rank, fields)

        with scope("w_land0"):
            tiles_land(n - 1, 0)

        @pl.when(is_hub)
        def _():
            with scope("w_plane"):
                wait_bytes(plane_proj.at[n - 1, 0:2 * len(plane_peers)], plane_recv.at[n - 1])
            value = sums_base[...] + jnp.dot(
                lead[0].reshape(cols * rank, 2 * width),
                plane_proj[n - 1].reshape(2 * width, fields),
                preferred_element_type=F32,
            ).reshape(cols, rank, fields)
            sums_out[n - 1] = value.astype(BF16).reshape(depths, 2, rank, fields)
            for i in range(depths - 1):
                if n < last:
                    sums_copy(n, far_depth(i)).start()
                else:
                    last_copy(far_depth(i), 0).start()
                    last_copy(far_depth(i), 1).start()
            if n == last:
                last_copy(my_z, 0).start()
            sums_in[n - 1, my_z] = sums_out[n - 1, my_z]

        with scope("w_tiles0"):
            tiles_close(n - 1, 0)
        with scope("tiles0"):
            near_tiles(n, 0)
        with scope("w_tiles1"):
            tiles_land(n - 1, 1)
        if n < last:
            with scope("older"):
                send_cores(n)
                send_older(n + 1)

        @pl.when(is_hub)
        def _():
            with scope("w_pairs"):
                wait_bytes(pairs.at[n - 1, 0:2 * (chips - 1)], pair_recv.at[n - 1])

        @pl.when(side == 0)
        def _():
            with scope("w_pairs"):
                wait_bytes(pairs.at[n - 1], pair_recv.at[n - 1])

        with scope("finish0"):
            near_finish(n, 0)
        with scope("w_tiles2"):
            tiles_close(n - 1, 1)
        with scope("finish1"):
            near_tiles(n, 1)
            near_finish(n, 1)
        if n == last:
            settle(n - 1)
            for d in range(len(peers)):
                energy_copy(0, d).start()

        if n < last:

            @pl.when(is_hub)
            def _():
                with scope("w_sums"):
                    wait_bytes(sums_in.at[n - 1, 0:depths - 1], sums_recv.at[n - 1])
                total = sums_in[n - 1, 0].astype(F32)
                for z in range(1, depths):
                    total += sums_in[n - 1, z].astype(F32)
                publish(n, total)

    @pl.when(side == 0)
    def _():
        with scope("w_last"):
            wait_bytes(first_in.at[0:depths], sums_recv.at[last - 1])

    @pl.when(is_hub)
    def _():
        with scope("w_last"):
            wait_bytes(first_in.at[0:depths - 1], sums_recv.at[last - 1])

    total = sums_in[last - 1, 0, side].astype(F32)
    for z in range(1, depths):
        total += sums_in[last - 1, z, side].astype(F32)
    pairs[last, my_row] = total.astype(BF16)
    settle(last)
    for d in range(len(peers)):
        energy_copy(1, d).start()
    energy_early[me] = energy_own[0:last]
    energy_last[me] = energy_own[last]
    for group, where in ((0, energy_early), (1, energy_last)):
        with scope("w_energy"):
            wait_bytes(where.at[0:len(peers)], energy_recv.at[group])
        total = where[0]
        for origin in range(1, rows * cols):
            total += where[origin]
        if group:
            energy_ref[last:last + 1, :] = total
        else:
            for n in range(last):
                energy_ref[n:n + 1, :] = total[n]

    with scope("w_sends"):
        wait_bytes(lifts.at[0:rows - 1], load_sems.at[1])
        wait_bytes(drive_tiles.at[:, :, 0:chips], history_sems.at[0])
        wait_bytes(drive_tiles.at[:, :, 0:chips - 1], history_sems.at[1])
        wait_bytes(energy_early.at[0:len(peers)], send_sems.at[0])
        wait_bytes(energy_last.at[0:len(peers)], send_sems.at[1])

        @pl.when(side == 0)
        def _():
            wait_bytes(first_in.at[0:cols], load_sems.at[0])
            wait_bytes(hub_cores.at[0:2], load_sems.at[3])
            wait_bytes(older_in.at[:, 0:2], load_sems.at[4])
            wait_bytes(drive.at[:, 0], load_sems.at[2])

        @pl.when(is_hub)
        def _():
            wait_bytes(first_in.at[0:cols - 1], load_sems.at[0])
            wait_bytes(hub_cores.at[0:1], load_sems.at[3])
            wait_bytes(older_in.at[:, 0:1], load_sems.at[4])
            wait_bytes(plane_proj.at[:, 0:2 * len(plane_peers)], load_sems.at[5])
            wait_bytes(plane_proj.at[:, 0:2 * (rows - 1)], load_sems.at[6])
            wait_bytes(sums_in.at[0:last - 1, 0:depths - 1], send_sems.at[2])
            wait_bytes(first_in.at[0:2 * depths - 1], load_sems.at[7])


def hand_over(steps_in, energy_in, steps_out, energy_out, sems):
    copies = (
        pltpu.make_async_copy(steps_in, steps_out, sems.at[0]),
        pltpu.make_async_copy(energy_in, energy_out, sems.at[1]),
    )
    for copy in copies:
        copy.start()
    for copy in copies:
        copy.wait()


def local(
    sources,
    history,
    inverse_diagonal,
    far_cores,
    target_basis,
    source_basis,
    near_blocks,
    near_tile,
    near_count,
):
    rows, _, lags, tile, fields = history.shape
    cols, rank = far_cores.shape[1:3]
    steps = sources.shape[2]
    slots = near_blocks.shape[2]
    panel_total = rows * cols * tile
    width = rows * rank
    depths = cols // 2
    lanes = min(128, tile, width)
    block = min(64, tile)
    dma = pltpu.SemaphoreType.DMA
    anywhere = pl.BlockSpec(memory_space=pltpu.HBM)
    inside = pl.BlockSpec(memory_space=pltpu.VMEM)
    new_steps, energies = pl.pallas_call(
        functools.partial(march, rows, cols, panel_total),
        out_shape=(
            pltpu.VMEM((steps, tile, fields), BF16),
            pltpu.VMEM((steps, fields), F32),
        ),
        in_specs=[anywhere] * 9,
        out_specs=(inside, inside),
        scratch_shapes=[
            pltpu.SMEM((1, 1, slots), jnp.int32),
            pltpu.SMEM((1, 1), jnp.int32),
            pltpu.VMEM((rows, rank, tile), BF16),
            pltpu.VMEM((rows, lags, tile, fields), BF16),
            pltpu.VMEM((2, depths * rank, lags * width), BF16),
            pltpu.VMEM((slots, tile, lags * tile), BF16),
            pltpu.VMEM((rank, tile), BF16),
            pltpu.VMEM((1, tile), F32),
            pltpu.VMEM((steps, tile, fields), BF16),
            pltpu.VMEM((tile, fields), F32),
            pltpu.VMEM((cols * rank, rows, lags, rank), BF16),
            pltpu.VMEM((slots, tile, lags, tile), BF16),
            pltpu.VMEM((max(2 * tile, width) // lanes, block * lags, lanes), F32),
            pltpu.VMEM((lags, rows, rank, fields), BF16),
            pltpu.VMEM((rows, rank, tile), BF16),
            pltpu.VMEM((tile, slots * rank), BF16),
            pltpu.VMEM((2 * rank, 2 * rank), BF16),
            pltpu.VMEM((4, steps - 1, depths * rank, width), BF16),
            pltpu.VMEM((steps - 1, cols, rank, 2 * width), BF16),
            pltpu.VMEM((steps - 1, 2, depths * rank, fields), BF16),
            pltpu.VMEM((steps - 1, 4, depths * rank, fields), BF16),
            pltpu.VMEM((2, depths, rank, fields), BF16),
            pltpu.VMEM((2 * cols, rank, fields), BF16),
            pltpu.VMEM((steps - 1, depths, 2, rank, fields), BF16),
            pltpu.VMEM((steps - 1, depths, 2, rank, fields), BF16),
            pltpu.VMEM((cols, rank, fields), F32),
            pltpu.VMEM((steps, rows, rank, fields), BF16),
            pltpu.VMEM((steps - 1, 2, rank, fields), F32),
            pltpu.VMEM((steps - 1, 2 * rows, rank, fields), BF16),
            pltpu.VMEM((steps - 1, 2, rows, tile, fields // 2), BF16),
            pltpu.VMEM((rows, tile, fields // 2), BF16),
            pltpu.VMEM((rows, rank, fields // 2), BF16),
            tuple(pltpu.VMEM((rows, tile, fields), BF16) for _ in range(steps - 1)),
            pltpu.VMEM((steps, tile, fields), F32),
            pltpu.VMEM((steps, 1, fields), F32),
            pltpu.VMEM((rows * cols, steps - 1, 1, fields), F32),
            pltpu.VMEM((rows * cols, 1, fields), F32),
            dma((8,)),
            dma(((lags + 1) // 2,)),
            dma((3,)),
            dma((2,)),
            dma((steps - 1,)),
            dma((steps - 1,)),
            dma((steps - 1,)),
            dma((steps - 1,)),
            dma((steps - 1,)),
            dma((steps - 1,)),
            dma((steps - 1, 2, rows // 2 - 1)),
            dma((steps - 1, 2)),
            dma((2,)),
        ],
        compiler_params=pltpu.CompilerParams(
            collective_id=0, has_side_effects=True, vmem_limit_bytes=63 * 1024 * 1024
        ),
    )(
        near_tile,
        near_count,
        jnp.swapaxes(source_basis[:, 0], 1, 2),
        history[:, 0],
        far_cores.reshape(cols * rank, rows, lags, rank),
        near_blocks[0, 0],
        jnp.swapaxes(target_basis[0, 0], 0, 1),
        inverse_diagonal[0],
        sources[0, 0],
    )
    new_steps, energies = pl.pallas_call(
        hand_over,
        out_shape=(
            jax.ShapeDtypeStruct((steps, tile, fields), BF16),
            jax.ShapeDtypeStruct((steps, fields), F32),
        ),
        in_specs=(inside, inside),
        out_specs=(anywhere, anywhere),
        scratch_shapes=[dma((2,))],
    )(
        pltpu.with_memory_space_constraint(new_steps, pltpu.VMEM),
        pltpu.with_memory_space_constraint(energies, pltpu.VMEM),
    )
    return new_steps[None, None], energies


def solution(mesh):
    placed = (
        P("row", "col", None, None, None),
        P(None, "col", None, None, None),
        P("row", "col", None),
        P("row", None, None, None, "col", None, None),
        P("row", "col", None, None),
        P(None, "col", None, None),
        P("row", "col", None, None, None, None),
        P("row", "col", None),
        P("row", "col"),
    )
    return jax.shard_map(
        local,
        mesh=mesh,
        in_specs=placed,
        out_specs=(P("row", "col", None, None, None), P()),
        check_vma=False,
    )
```

```python
import contextlib
import functools

import jax
import jax.numpy as jnp
from jax import lax
from jax.experimental import pallas as pl
from jax.experimental.pallas import tpu as pltpu
from jax.sharding import PartitionSpec as P

MESH = pl.DeviceIdType.MESH
F32 = jnp.float32
BF16 = jnp.bfloat16
scope = contextlib.nullcontext


def march(
    rows,
    cols,
    panel_total,
    tiles_hbm,
    count_hbm,
    basis_hbm,
    history_hbm,
    cores_hbm,
    near_hbm,
    target_hbm,
    scaling_hbm,
    sources_hbm,
    steps_ref,
    energy_ref,
    tiles_ref,
    count_ref,
    basis,
    history,
    cores,
    near_blocks,
    target,
    scaling_row,
    sources,
    scaling,
    cores_raw,
    near_raw,
    stage,
    past_proj,
    lifts,
    weave,
    mixer,
    hub_cores,
    lead,
    older_out,
    older_in,
    first_out,
    first_in,
    sums_out,
    sums_in,
    sums_base,
    pairs,
    drive,
    plane_proj,
    drive_tiles,
    tile_pool,
    core_pool,
    fresh_tiles,
    near_sum,
    energy_own,
    energy_early,
    energy_last,
    load_sems,
    history_sems,
    send_sems,
    start_recv,
    cores_recv,
    older_recv,
    drive_recv,
    plane_recv,
    pair_recv,
    sums_recv,
    tile_recv,
    pass_recv,
    energy_recv,
):
    step_count = sources.shape[0]
    lag_count, _, rank, fields = past_proj.shape
    tile = history.shape[2]
    slot_count = near_blocks.shape[0]
    width = rows * rank
    chips = rows // 2
    depths = cols // 2
    my_row = lax.axis_index("row")
    my_col = lax.axis_index("col")
    side = lax.rem(my_row, 2)
    chip = my_row // 2
    my_z = my_col // 2
    my_x = lax.rem(my_col, 2)
    partner = my_row + 1 - 2 * side
    hub_row = 2 * chip + 1
    is_hub = side == 1
    own_pair = pl.ds(2 * chip, 2)
    plane_pair = pl.ds(my_x * rows + 2 * chip, 2)
    me = my_row * cols + my_col

    def row_peer(d):
        return lax.rem(my_row + d, rows)

    def col_peer(d):
        return lax.rem(my_col + d, cols)

    def far_depth(i):
        up = i + (i - my_z + depths) // depths
        mirrored = depths - 1 - my_z
        down = depths - 1 - (i + (i - mirrored + depths) // depths)
        upper = 2 * my_z // depths
        return upper * up + (1 - upper) * down

    loads = [
        pltpu.make_async_copy(src, dst, load_sems.at[n])
        for n, (src, dst) in enumerate(
            (
                (basis_hbm, basis),
                (cores_hbm, cores_raw),
                (near_hbm, near_raw),
                (target_hbm, target),
                (scaling_hbm, scaling_row),
                (sources_hbm, sources),
                (tiles_hbm, tiles_ref),
                (count_hbm, count_ref),
            )
        )
    ]
    spans = [(lag, min(2, lag_count - lag)) for lag in range(0, lag_count, 2)]

    def history_load(index):
        first, length = spans[index]
        return pltpu.make_async_copy(
            history_hbm.at[:, first:first + length],
            history.at[:, first:first + length],
            history_sems.at[index],
        )

    def wait_bytes(ref, sem):
        pltpu.make_async_copy(ref, ref, sem).wait()

    for load in (loads[1], loads[0], *loads[3:5]):
        load.start()
    for index in range(len(spans)):
        history_load(index).start()

    barrier = pltpu.get_barrier_semaphore()
    peers = [(a, b) for a in range(rows) for b in range(cols) if a or b]

    def greet(index, carry):
        pl.semaphore_signal(
            barrier, inc=1, device_id=(row_peer(index // cols), col_peer(lax.rem(index, cols))),
            device_id_type=MESH,
        )
        return carry

    lax.fori_loop(1, rows * cols, greet, 0)

    def copy_to(src, dst, send, recv, row, col):
        return pltpu.make_async_remote_copy(
            src_ref=src, dst_ref=dst, send_sem=send, recv_sem=recv,
            device_id=(row, col), device_id_type=MESH,
        )

    def first_copy(z, x):
        return copy_to(
            first_out.at[x, z], first_in.at[side * cols + my_col],
            load_sems.at[0], start_recv.at[0], hub_row, z * 2 + x,
        )

    def cores_copy(k, x):
        return copy_to(
            cores.at[x, :, k * width:(k + 1) * width], hub_cores.at[my_x * 2 + side, k],
            load_sems.at[3], cores_recv.at[k], hub_row, my_z * 2 + x,
        )

    def lift_copy(d):
        return copy_to(
            lifts.at[my_row], lifts.at[my_row],
            load_sems.at[1], start_recv.at[1], row_peer(d), my_col,
        )

    def older_copy(n, x):
        return copy_to(
            older_out.at[n - 1, x], older_in.at[n - 1, my_x * 2 + side],
            load_sems.at[4], older_recv.at[n - 1], hub_row, my_z * 2 + x,
        )

    def drive_copy(n):
        return copy_to(
            drive.at[n, 0], drive.at[n, 0], load_sems.at[2], drive_recv.at[n], hub_row, my_col
        )

    def plane_copy(n, dy, dx):
        return copy_to(
            plane_proj.at[n, plane_pair], plane_proj.at[n, plane_pair],
            load_sems.at[5], plane_recv.at[n],
            2 * lax.rem(chip + dy, chips) + 1, my_z * 2 + lax.rem(my_x + dx, 2),
        )

    def pair_copy(n, d):
        return copy_to(
            pairs.at[n, own_pair], pairs.at[n, own_pair],
            load_sems.at[6], pair_recv.at[n], row_peer(d), my_col,
        )

    def sums_copy(n, z):
        return copy_to(
            sums_out.at[n - 1, z], sums_in.at[n - 1, my_z],
            send_sems.at[3], sums_recv.at[n - 1], my_row, z * 2 + my_x,
        )

    def last_copy(z, c):
        return copy_to(
            sums_out.at[step_count - 2, z, c], sums_in.at[step_count - 2, my_z, c],
            load_sems.at[7], sums_recv.at[step_count - 2], hub_row - 1 + c, z * 2 + my_x,
        )

    def tile_copy(n, part, owner, to, index):
        return copy_to(
            drive_tiles.at[n, part, owner], drive_tiles.at[n, part, owner],
            history_sems.at[0],
            pass_recv.at[n, part] if index is None else tile_recv.at[n, part, index],
            to, my_col,
        )

    def pass_copy(n, part, owner):
        return copy_to(
            drive_tiles.at[n, part, owner], drive_tiles.at[n, part, owner],
            history_sems.at[1], pass_recv.at[n, part], partner, my_col,
        )

    def energy_copy(last, d):
        return copy_to(
            energy_own.at[step_count - 3 + last] if last else energy_own.at[0:step_count - 2],
            energy_last.at[last - 1, me] if last else energy_early.at[me],
            send_sems.at[last], energy_recv.at[last],
            row_peer(peers[d][0]), col_peer(peers[d][1]),
        )

    plane_peers = [(dy, dx) for dy in reversed(range(chips)) for dx in (1, 0) if dy or dx]

    def far_sum(n, x):
        depth = lag_count - n
        return jnp.dot(
            cores[x, :, n * width:],
            past_proj[0:depth].reshape(depth * width, fields),
            preferred_element_type=F32,
        ).astype(BF16)

    def near_base(n):
        depth = lag_count - n

        def add_slot(slot, carry):
            where = tiles_ref[0, 0, slot]
            value = jnp.dot(
                near_blocks[slot, :, n * tile:],
                history[where, 0:depth].reshape(depth * tile, fields),
                preferred_element_type=F32,
            )
            for lag in range(1, n):
                value += jnp.dot(
                    near_blocks[slot, :, lag * tile:(lag + 1) * tile],
                    fresh_tiles[n - 1 - lag][where],
                    preferred_element_type=F32,
                )
            near_sum[n] += value
            return carry

        near_sum[n] = jnp.zeros((tile, fields), F32)
        lax.fori_loop(0, slot_count, add_slot, 0)

    half = fields // 2

    def send_tiles(n, part):
        for d in range(2, rows, 2):
            tile_copy(n, part, my_row, row_peer(d), (rows - d) // 2 - 1).start()

    def near_tiles(n, part):
        here = slice(part * half, (part + 1) * half)
        tile_pool[...] = drive_tiles[n - 1, part]
        total = near_sum[n, :, here]
        for slot in range(slot_count):
            total += jnp.dot(
                near_blocks[slot, :, 0:tile],
                tile_pool[tiles_ref[0, 0, slot]],
                preferred_element_type=F32,
            )
        near_sum[n, :, here] = total

    def near_first():
        driven = scaling[...] * (sources[0].astype(F32) - near_sum[0])
        near_sum[0] = driven
        sent = driven.astype(BF16)
        drive[0, side] = jnp.dot(basis[my_row], sent, preferred_element_type=F32)

        @pl.when(side == 0)
        def _():
            drive_copy(0).start()

        for part in range(2):
            drive_tiles[0, part, my_row] = sent[:, part * half:(part + 1) * half]
        send_tiles(0, 0)

        @pl.when(side == 0)
        def _():
            send_tiles(0, 1)

        for part in range(2):
            tile_copy(0, part, my_row, partner, None).start()

    def near_finish(n, part):
        here = slice(part * half, (part + 1) * half)
        core_pool[...] = pairs[n - 1, :, :, here]
        known = [core_pool[tiles_ref[0, 0, slot]] for slot in range(slot_count)]
        total = near_sum[n, :, here] - jnp.dot(
            weave[...], jnp.concatenate(known, axis=0), preferred_element_type=F32
        )
        driven = scaling[:, here] * (sources[n, :, here].astype(F32) - total)
        near_sum[n, :, here] = driven
        if n + 1 < step_count:
            sent = driven.astype(BF16)
            drive_tiles[n, part, my_row] = sent
            if part == 0:
                send_tiles(n, part)
            else:

                @pl.when(side == 0)
                def _():
                    send_tiles(n, part)

            tile_copy(n, part, my_row, partner, None).start()
            drive[n, side, :, here] = jnp.dot(
                basis[my_row], sent, preferred_element_type=F32
            )
            if part == 1:

                @pl.when(side == 0)
                def _():
                    drive_copy(n).start()

    def tiles_land(n, part):
        for d in range(2, rows, 2):
            tile_copy(n, part, row_peer(d), partner, d // 2 - 1).wait_recv()
            pass_copy(n, part, row_peer(d)).start()

    def tiles_close(n, part):
        wait_bytes(drive_tiles.at[n, part, 0:chips], pass_recv.at[n, part])

    def settle(n):
        far = lax.dot_general(
            target[...], pairs[n, my_row], (((0,), (0,)), ((), ())), preferred_element_type=F32
        )
        fresh = (near_sum[n] - scaling[...] * far).astype(BF16)
        energy_own[n] = (
            jnp.sum(jnp.square(fresh.astype(F32)), axis=0, keepdims=True) / panel_total
        )
        steps_ref[n] = fresh
        if n + 1 < step_count:
            fresh_tiles[n][my_row] = fresh

    def rebuild(n):
        for d in range(1, rows):
            p = row_peer(d)
            far = lax.dot_general(
                lifts[p], pairs[n, p], (((0,), (0,)), ((), ())), preferred_element_type=F32
            )
            for part in range(2):
                here = slice(part * half, (part + 1) * half)
                fresh_tiles[n][p, :, here] = (
                    drive_tiles[n, part, p].astype(F32) - far[:, here]
                ).astype(BF16)

    def publish(n, core):
        mine = core.astype(BF16)
        pairs[n, own_pair] = mine
        wait_bytes(drive.at[n, 0], drive_recv.at[n])
        mixed = jnp.dot(
            mixer[...], mine.reshape(2 * rank, fields), preferred_element_type=F32
        )
        plane_proj[n, plane_pair] = (
            drive[n] - mixed.reshape(2, rank, fields)
        ).astype(BF16)
        for dy, dx in plane_peers:
            plane_copy(n, dy, dx).start()
        for d in (rows - 1, *range(1, rows - 1, 2)):
            pair_copy(n, d).start()
        send_tiles(n, 1)
        for d in range(2, rows - 1, 2):
            pair_copy(n, d).start()

    lanes = stage.shape[2]
    block = stage.shape[1] // lag_count

    def spread(value, base=0):
        for c in range(value.shape[1] // lanes):
            stage[base + c, 0:value.shape[0]] = value[:, c * lanes:(c + 1) * lanes]

    def pick(lag, c, length):
        return stage[c, pl.ds(lag, length, stride=lag_count), :].astype(BF16)

    def pack_cores(z):
        span = 2 * rank
        here = pl.ds(z * span, span)
        base = z % (stage.shape[0] * lanes // width) * (width // lanes)
        total = None
        for p in range(rows):
            value = cores_raw[here, p].astype(F32).reshape(span * lag_count, rank).astype(BF16)
            place = (
                lax.broadcasted_iota(jnp.int32, (rank, width), 1)
                == lax.broadcasted_iota(jnp.int32, (rank, width), 0) + p * rank
            )
            term = jnp.dot(
                value, place.astype(F32).astype(BF16), preferred_element_type=F32
            )
            total = term if total is None else total + term
        spread(total, base)
        for lag in range(lag_count):
            for c in range(width // lanes):
                first = lag * width + c * lanes
                both = pick(lag, base + c, span)
                for x in range(2):
                    cores[x, z * rank:(z + 1) * rank, first:first + lanes] = (
                        both[x * rank:(x + 1) * rank]
                    )

    def pack_block(index, base):
        slot = index // (tile // block)
        here = pl.ds(pl.multiple_of(lax.rem(index, tile // block) * block, block), block)
        spread(near_raw[slot, here].astype(F32).reshape(block * lag_count, tile), base)
        for lag in range(lag_count):
            for c in range(tile // lanes):
                first = lag * tile + c * lanes
                near_blocks[slot, here, first:first + lanes] = jnp.where(
                    slot < count_ref[0, 0], pick(lag, base + c, block), jnp.zeros((block, lanes), BF16)
                )

    turns = stage.shape[0] * lanes // tile

    def pack_near(index, carry):
        for turn in range(turns):
            pack_block(index * turns + turn, turn * (tile // lanes))
        return carry

    with scope("w_cores"):
        loads[1].wait()
        for load in (loads[2], *loads[5:]):
            load.start()
    with scope("pack_cores"):
        for z in range(depths):
            pack_cores(z)
        loads[0].wait()
    with scope("project"):
        for index, (first, length) in enumerate(spans):
            history_load(index).wait()
            for lag in range(first, first + length):
                for p in range(rows):
                    past_proj[lag, p] = jnp.dot(
                        basis[p], history[p, lag], preferred_element_type=F32
                    ).astype(BF16)

    for x in range(2):
        first_out[x] = far_sum(0, x).reshape(depths, rank, fields)
    with scope("barrier"):
        pl.semaphore_wait(barrier, rows * cols - 1)
    for i in range(depths - 1):
        for x in (1 - my_x, my_x):
            first_copy(far_depth(i), x).start()
    first_copy(my_z, 1 - my_x).start()

    @pl.when(is_hub)
    def _():
        first_in[cols + my_col] = first_out[my_x, my_z]

    @pl.when(side == 0)
    def _():
        first_copy(my_z, my_x).start()

    for load in loads[3:5]:
        load.wait()
    lifts[my_row] = (target[...].astype(F32) * scaling_row[...]).astype(BF16)
    for d in range(1, rows):
        lift_copy(d).start()

    def send_older(n):
        for x in range(2):
            older_out[n - 1, x] = far_sum(n, x)
        older_copy(n, 1 - my_x).start()

        @pl.when(side == 0)
        def _():
            older_copy(n, my_x).start()

        @pl.when(is_hub)
        def _():
            older_in[n - 1, my_x * 2 + 1] = older_out[n - 1, my_x]

    def send_cores(k):
        cores_copy(k, 1 - my_x).start()

        @pl.when(side == 0)
        def _():
            cores_copy(k, my_x).start()

        @pl.when(is_hub)
        def _():
            hub_cores[my_x * 2 + 1, k] = cores[my_x, :, k * width:(k + 1) * width]

    with scope("older1"):
        send_cores(0)
        send_older(1)
    with scope("pack_near"):
        for load in (loads[2], *loads[6:]):
            load.wait()
        lax.fori_loop(0, slot_count * (tile // block) // turns, pack_near, 0)
    with scope("near_base0"):
        near_base(0)
    with scope("near0"):
        loads[5].wait()
        scaling[...] = jnp.transpose(jnp.broadcast_to(scaling_row[...], (fields, tile)))
        near_first()
    with scope("w_lifts"):
        wait_bytes(lifts.at[0:rows - 1], start_recv.at[1])
    weave[...] = jnp.concatenate(
        [
            lax.dot_general(
                near_blocks[slot, :, 0:tile], lifts[tiles_ref[0, 0, slot]],
                (((1,), (1,)), ((), ())), preferred_element_type=F32,
            )
            for slot in range(slot_count)
        ],
        axis=1,
    ).astype(BF16)

    @pl.when(is_hub)
    def _():
        for c in range(2):
            own = lax.dot_general(
                basis[2 * chip + c], lifts[2 * chip + c], (((1,), (1,)), ((), ())),
                preferred_element_type=F32,
            ).astype(BF16)
            none = jnp.zeros((rank, rank), BF16)
            mixer[c * rank:(c + 1) * rank] = jnp.concatenate(
                [own, none] if c == 0 else [none, own], axis=1
            )
        with scope("w_first"):
            wait_bytes(first_in.at[0:2 * cols - 1], start_recv.at[0])
        core = []
        for c in range(2):
            total = first_in[c * cols].astype(F32)
            for j in range(1, cols):
                total += first_in[c * cols + j].astype(F32)
            core.append(total)
        publish(0, jnp.stack(core))

    def lead_rows(k):
        for z in range(depths):
            for c in range(2):
                for x in range(2):
                    lead[k, z * 2 + c, :, x * width:(x + 1) * width] = hub_cores[
                        x * 2 + c, k, z * rank:(z + 1) * rank
                    ]

    last = step_count - 1
    for n in range(1, step_count):
        if n > 1:
            with scope("settle"):
                settle(n - 2)
                rebuild(n - 2)
            if n == last:
                for d in range(len(peers)):
                    energy_copy(0, d).start()
        with scope("near_base"):
            near_base(n)

        @pl.when(is_hub)
        def _():
            with scope("base"):
                wait_bytes(hub_cores.at[0:3, n - 1], cores_recv.at[n - 1])
                lead_rows(n - 1)
                wait_bytes(older_in.at[n - 1, 0:3], older_recv.at[n - 1])
                for z in range(depths):
                    for c in range(2):
                        here = slice(z * rank, (z + 1) * rank)
                        sums_base[z * 2 + c] = older_in[n - 1, c, here].astype(
                            F32
                        ) + older_in[n - 1, 2 + c, here].astype(F32)
                for lag in range(1, n):
                    sums_base[...] += jnp.dot(
                        lead[lag].reshape(cols * rank, 2 * width),
                        plane_proj[n - 1 - lag].reshape(2 * width, fields),
                        preferred_element_type=F32,
                    ).reshape(cols, rank, fields)

        with scope("w_land0"):
            tiles_land(n - 1, 0)

        @pl.when(is_hub)
        def _():
            with scope("w_plane"):
                wait_bytes(plane_proj.at[n - 1, 0:2 * len(plane_peers)], plane_recv.at[n - 1])
            value = sums_base[...] + jnp.dot(
                lead[0].reshape(cols * rank, 2 * width),
                plane_proj[n - 1].reshape(2 * width, fields),
                preferred_element_type=F32,
            ).reshape(cols, rank, fields)
            sums_out[n - 1] = value.astype(BF16).reshape(depths, 2, rank, fields)
            for i in range(depths - 1):
                if n < last:
                    sums_copy(n, far_depth(i)).start()
                else:
                    last_copy(far_depth(i), 0).start()
                    last_copy(far_depth(i), 1).start()
            if n == last:
                last_copy(my_z, 0).start()
            sums_in[n - 1, my_z] = sums_out[n - 1, my_z]

        with scope("w_tiles0"):
            tiles_close(n - 1, 0)
        with scope("tiles0"):
            near_tiles(n, 0)
        with scope("w_tiles1"):
            tiles_land(n - 1, 1)
        if n < last:
            with scope("older"):
                send_cores(n)
                send_older(n + 1)

        @pl.when(is_hub)
        def _():
            with scope("w_pairs"):
                wait_bytes(pairs.at[n - 1, 0:2 * (chips - 1)], pair_recv.at[n - 1])

        @pl.when(side == 0)
        def _():
            with scope("w_pairs"):
                wait_bytes(pairs.at[n - 1], pair_recv.at[n - 1])

        with scope("finish0"):
            near_finish(n, 0)
        with scope("w_tiles2"):
            tiles_close(n - 1, 1)
        with scope("finish1"):
            near_tiles(n, 1)
            near_finish(n, 1)
        if n == last:
            settle(n - 1)
            for d in range(len(peers)):
                energy_copy(1, d).start()

        if n < last:

            @pl.when(is_hub)
            def _():
                with scope("w_sums"):
                    wait_bytes(sums_in.at[n - 1, 0:depths - 1], sums_recv.at[n - 1])
                total = sums_in[n - 1, 0].astype(F32)
                for z in range(1, depths):
                    total += sums_in[n - 1, z].astype(F32)
                publish(n, total)

    @pl.when(side == 0)
    def _():
        with scope("w_last"):
            wait_bytes(first_in.at[0:depths], sums_recv.at[last - 1])

    @pl.when(is_hub)
    def _():
        with scope("w_last"):
            wait_bytes(first_in.at[0:depths - 1], sums_recv.at[last - 1])

    total = sums_in[last - 1, 0, side].astype(F32)
    for z in range(1, depths):
        total += sums_in[last - 1, z, side].astype(F32)
    pairs[last, my_row] = total.astype(BF16)
    settle(last)
    for d in range(len(peers)):
        energy_copy(2, d).start()
    energy_early[me] = energy_own[0:last - 1]
    energy_last[0, me] = energy_own[last - 1]
    energy_last[1, me] = energy_own[last]
    for group, where in enumerate((energy_early, energy_last.at[0], energy_last.at[1])):
        wait_bytes(where.at[0:len(peers)], energy_recv.at[group])
        total = where[0]
        for origin in range(1, rows * cols):
            total += where[origin]
        if group:
            energy_ref[last - 2 + group:last - 1 + group, :] = total
        else:
            for n in range(last - 1):
                energy_ref[n:n + 1, :] = total[n]

    with scope("w_sends"):
        wait_bytes(lifts.at[0:rows - 1], load_sems.at[1])
        wait_bytes(drive_tiles.at[:, :, 0:chips], history_sems.at[0])
        wait_bytes(drive_tiles.at[:, :, 0:chips - 1], history_sems.at[1])
        wait_bytes(energy_early.at[0:len(peers)], send_sems.at[0])
        wait_bytes(energy_last.at[0, 0:len(peers)], send_sems.at[1])
        wait_bytes(energy_last.at[1, 0:len(peers)], send_sems.at[2])

        @pl.when(side == 0)
        def _():
            wait_bytes(first_in.at[0:cols], load_sems.at[0])
            wait_bytes(hub_cores.at[0:2], load_sems.at[3])
            wait_bytes(older_in.at[:, 0:2], load_sems.at[4])
            wait_bytes(drive.at[:, 0], load_sems.at[2])

        @pl.when(is_hub)
        def _():
            wait_bytes(first_in.at[0:cols - 1], load_sems.at[0])
            wait_bytes(hub_cores.at[0:1], load_sems.at[3])
            wait_bytes(older_in.at[:, 0:1], load_sems.at[4])
            wait_bytes(plane_proj.at[:, 0:2 * len(plane_peers)], load_sems.at[5])
            wait_bytes(plane_proj.at[:, 0:2 * (rows - 1)], load_sems.at[6])
            wait_bytes(sums_in.at[0:last - 1, 0:depths - 1], send_sems.at[3])
            wait_bytes(first_in.at[0:2 * depths - 1], load_sems.at[7])


def hand_over(steps_in, energy_in, steps_out, energy_out, sems):
    copies = (
        pltpu.make_async_copy(steps_in, steps_out, sems.at[0]),
        pltpu.make_async_copy(energy_in, energy_out, sems.at[1]),
    )
    for copy in copies:
        copy.start()
    for copy in copies:
        copy.wait()


def local(
    sources,
    history,
    inverse_diagonal,
    far_cores,
    target_basis,
    source_basis,
    near_blocks,
    near_tile,
    near_count,
):
    rows, _, lags, tile, fields = history.shape
    cols, rank = far_cores.shape[1:3]
    steps = sources.shape[2]
    slots = near_blocks.shape[2]
    panel_total = rows * cols * tile
    width = rows * rank
    depths = cols // 2
    lanes = min(128, tile, width)
    block = min(64, tile)
    dma = pltpu.SemaphoreType.DMA
    anywhere = pl.BlockSpec(memory_space=pltpu.HBM)
    inside = pl.BlockSpec(memory_space=pltpu.VMEM)
    new_steps, energies = pl.pallas_call(
        functools.partial(march, rows, cols, panel_total),
        out_shape=(
            pltpu.VMEM((steps, tile, fields), BF16),
            pltpu.VMEM((steps, fields), F32),
        ),
        in_specs=[anywhere] * 9,
        out_specs=(inside, inside),
        scratch_shapes=[
            pltpu.SMEM((1, 1, slots), jnp.int32),
            pltpu.SMEM((1, 1), jnp.int32),
            pltpu.VMEM((rows, rank, tile), BF16),
            pltpu.VMEM((rows, lags, tile, fields), BF16),
            pltpu.VMEM((2, depths * rank, lags * width), BF16),
            pltpu.VMEM((slots, tile, lags * tile), BF16),
            pltpu.VMEM((rank, tile), BF16),
            pltpu.VMEM((1, tile), F32),
            pltpu.VMEM((steps, tile, fields), BF16),
            pltpu.VMEM((tile, fields), F32),
            pltpu.VMEM((cols * rank, rows, lags, rank), BF16),
            pltpu.VMEM((slots, tile, lags, tile), BF16),
            pltpu.VMEM((max(2 * tile, width) // lanes, block * lags, lanes), F32),
            pltpu.VMEM((lags, rows, rank, fields), BF16),
            pltpu.VMEM((rows, rank, tile), BF16),
            pltpu.VMEM((tile, slots * rank), BF16),
            pltpu.VMEM((2 * rank, 2 * rank), BF16),
            pltpu.VMEM((4, steps - 1, depths * rank, width), BF16),
            pltpu.VMEM((steps - 1, cols, rank, 2 * width), BF16),
            pltpu.VMEM((steps - 1, 2, depths * rank, fields), BF16),
            pltpu.VMEM((steps - 1, 4, depths * rank, fields), BF16),
            pltpu.VMEM((2, depths, rank, fields), BF16),
            pltpu.VMEM((2 * cols, rank, fields), BF16),
            pltpu.VMEM((steps - 1, depths, 2, rank, fields), BF16),
            pltpu.VMEM((steps - 1, depths, 2, rank, fields), BF16),
            pltpu.VMEM((cols, rank, fields), F32),
            pltpu.VMEM((steps, rows, rank, fields), BF16),
            pltpu.VMEM((steps - 1, 2, rank, fields), F32),
            pltpu.VMEM((steps - 1, 2 * rows, rank, fields), BF16),
            pltpu.VMEM((steps - 1, 2, rows, tile, fields // 2), BF16),
            pltpu.VMEM((rows, tile, fields // 2), BF16),
            pltpu.VMEM((rows, rank, fields // 2), BF16),
            tuple(pltpu.VMEM((rows, tile, fields), BF16) for _ in range(steps - 1)),
            pltpu.VMEM((steps, tile, fields), F32),
            pltpu.VMEM((steps, 1, fields), F32),
            pltpu.VMEM((rows * cols, steps - 2, 1, fields), F32),
            pltpu.VMEM((2, rows * cols, 1, fields), F32),
            dma((8,)),
            dma(((lags + 1) // 2,)),
            dma((4,)),
            dma((2,)),
            dma((steps - 1,)),
            dma((steps - 1,)),
            dma((steps - 1,)),
            dma((steps - 1,)),
            dma((steps - 1,)),
            dma((steps - 1,)),
            dma((steps - 1, 2, rows // 2 - 1)),
            dma((steps - 1, 2)),
            dma((3,)),
        ],
        compiler_params=pltpu.CompilerParams(
            collective_id=0, has_side_effects=True, vmem_limit_bytes=63 * 1024 * 1024
        ),
    )(
        near_tile,
        near_count,
        jnp.swapaxes(source_basis[:, 0], 1, 2),
        history[:, 0],
        far_cores.reshape(cols * rank, rows, lags, rank),
        near_blocks[0, 0],
        jnp.swapaxes(target_basis[0, 0], 0, 1),
        inverse_diagonal[0],
        sources[0, 0],
    )
    new_steps, energies = pl.pallas_call(
        hand_over,
        out_shape=(
            jax.ShapeDtypeStruct((steps, tile, fields), BF16),
            jax.ShapeDtypeStruct((steps, fields), F32),
        ),
        in_specs=(inside, inside),
        out_specs=(anywhere, anywhere),
        scratch_shapes=[dma((2,))],
    )(
        pltpu.with_memory_space_constraint(new_steps, pltpu.VMEM),
        pltpu.with_memory_space_constraint(energies, pltpu.VMEM),
    )
    return new_steps[None, None], energies


def solution(mesh):
    placed = (
        P("row", "col", None, None, None),
        P(None, "col", None, None, None),
        P("row", "col", None),
        P("row", None, None, None, "col", None, None),
        P("row", "col", None, None),
        P(None, "col", None, None),
        P("row", "col", None, None, None, None),
        P("row", "col", None),
        P("row", "col"),
    )
    return jax.shard_map(
        local,
        mesh=mesh,
        in_specs=placed,
        out_specs=(P("row", "col", None, None, None), P()),
        check_vma=False,
    )
```
